32 devices in a mesh: lat: 16 (over z, y, x), lev: 2 (over core).
Axes of the slice: x: 2, y: 2, z: 4, core: 2. Of those that a mesh axis runs over, the one named last changes fastest.
Arguments:
- fields: float32 [160, 3, 16, 2560], P('lat', None, 'lev'), may hold values from 0.1 to 5
- lat_fraction: float32 [160], P('lat'), may hold values from 0 to 1
- lon_fraction: float32 [160], P('lat'), may hold values from 0 to 1
- lon_shift: int32 [160], P('lat'), may hold values from 0 to 2559
- departure_row: int32 [160], P('lat'), may hold values from 1 to 157, as said below
- extents: int32 [16, 2], P('lat'), may hold values from 1 to 4
Outputs:
- advected: float32 [160, 3, 16, 2560], P('lat', None, 'lev')
The draws below stay inside these ranges and needn't reach their ends.
Inputs may be any that keep to these rules, and one draw needn't show every extreme that they name: departure_row[r] lies within 39 rows of r.
All inputs are finite; a program needn't handle non-finite values.
Results may differ from the reference program's by a relative error of at most 0.0003.
Values sent between devices are 32-bit elements; how exact they have to be, the bound alone decides.
A program may use at most 128 MiB of HBM per device.

```python
import math
import jax
import jax.numpy as jnp
from jax import lax

ROWS = 10
LON = 2560
FIELDS = 3
REACH = 4
NLAT = 160
LEV = 16
BANDS = 16


def band_phase(key):
    return jax.random.randint(jax.random.fold_in(key, 911), (), 0, 8 * ROWS)


def draw_fields(key, part):
    row_phase = band_phase(key)
    shifted_rows = (jnp.arange(NLAT, dtype=jnp.int32) + row_phase) % (8 * ROWS)
    row_angle = 2.0 * math.pi * shifted_rows.astype(jnp.float32) / (8 * ROWS)
    full_shape = (NLAT, FIELDS, LEV, LON)
    gain_row = jnp.exp(-0.5 * jnp.sin(row_angle))
    rough_part = jax.random.uniform(jax.random.fold_in(key, 23), full_shape, jnp.float32, 0.5, 2.0)
    return (gain_row[:, None, None, None] * rough_part).astype(jnp.float32)


def draw_departure_row(key, part):
    row_phase = band_phase(key)
    row_ids = jnp.arange(NLAT, dtype=jnp.int32)
    shifted_rows = (row_ids + row_phase) % (8 * ROWS)
    row_drift = jnp.clip(2 * (2 * ROWS - jnp.abs(shifted_rows - 4 * ROWS)), -2 * ROWS, 2 * ROWS)
    row_noise = jax.random.randint(jax.random.fold_in(key, 17), (NLAT,), -2 * ROWS, 2 * ROWS + 1)
    offsets = jnp.clip(row_drift + row_noise, -REACH * ROWS + 1, REACH * ROWS - 2)
    spread = jax.random.randint(jax.random.fold_in(key, 29), (NLAT,), 0, 1 << 20)
    north_offset = -(1 + spread % (REACH * ROWS - 1))
    south_offset = 1 + spread % (REACH * ROWS - 2)
    position = row_ids % ROWS
    offsets = jnp.where(position == 0, north_offset, offsets)
    offsets = jnp.where(position == ROWS - 1, south_offset, offsets)
    return jnp.clip(row_ids + offsets, 1, NLAT - 3).astype(jnp.int32)


def plant(array, rng, low, largest):
    spot = [jax.random.randint(jax.random.fold_in(rng, axis), (), 0, length) for axis, length in enumerate(array.shape)]
    widest = array.shape.index(max(array.shape))
    next_to = spot[:widest] + [(spot[widest] + 1) % array.shape[widest]] + spot[widest + 1:]
    return array.at[tuple(spot)].set(low).at[tuple(next_to)].set(largest)


def level_of(stream_key, shape, pieces, smallest, high):
    def one(axis_at, blocks):
        heights = jax.random.uniform(jax.random.fold_in(jax.random.fold_in(stream_key, 6), axis_at), (blocks,), jnp.float32, smallest / len(pieces), high / len(pieces))
        return jnp.repeat(jnp.exp(heights), shape[axis_at] // blocks).reshape((-1,) + (1,) * (len(shape) - axis_at - 1))

    gain = one(*pieces[0])
    for cut in pieces[1:]:
        gain = gain * one(*cut)
    return gain


def setup_inputs(seed: int = 0) -> dict:
    key_of = jax.random.split(jax.random.key(seed), 7)
    return {
        "fields": draw_fields(jax.random.fold_in(key_of[6], 71), 0),
        "lat_fraction": jnp.clip(1.0 * jax.random.uniform(key_of[1], (NLAT,), jnp.float32) ** level_of(key_of[1], (NLAT,), ((0, 16),), -0.2, 0.2), 0.0, 1.0),
        "lon_fraction": jnp.clip(1.0 * jax.random.uniform(key_of[2], (NLAT,), jnp.float32) ** level_of(key_of[2], (NLAT,), ((0, 16),), -0.2, 0.2), 0.0, 1.0),
        "lon_shift": plant(jax.random.randint(key_of[3], (NLAT,), 0, LON), jax.random.fold_in(key_of[3], 1), 0, LON - 1).astype(jnp.int32),
        "departure_row": draw_departure_row(jax.random.fold_in(key_of[6], 71), 0),
        "extents": plant(jax.random.randint(key_of[5], (BANDS, 2), 1, REACH + 1), jax.random.fold_in(key_of[5], 1), 1, REACH).astype(jnp.int32),
    }


def cubic_weights(fraction):
    return jnp.stack([-fraction * (fraction - 1.0) * (fraction - 2.0) / 6.0,
                      (fraction + 1.0) * (fraction - 1.0) * (fraction - 2.0) / 2.0,
                      -(fraction + 1.0) * fraction * (fraction - 2.0) / 2.0,
                      (fraction + 1.0) * fraction * (fraction - 1.0) / 6.0])


def along_lon(column, lon_w, shift_value):
    lon_count = column.shape[-1]
    doubled = jnp.concatenate([column, column], axis=-1)
    result = jnp.zeros_like(column)
    for offset in range(4):
        first = ((shift_value + offset - 1) % lon_count).astype(jnp.int32)
        result = result + lon_w[offset] * lax.dynamic_slice_in_dim(doubled, first, lon_count, 2)
    return result


def reference(fields, lat_fraction, lon_fraction, lon_shift, departure_row, extents):
    row_ids = jnp.arange(NLAT, dtype=jnp.int32)
    band_ids = row_ids // ROWS
    low_bound = band_ids * ROWS - extents[band_ids, 0] * ROWS + 1
    high_bound = band_ids * ROWS + ROWS - 3 + extents[band_ids, 1] * ROWS
    departure = jnp.clip(jnp.clip(departure_row, low_bound, high_bound), 1, NLAT - 3).astype(jnp.int32)

    def one_row(inputs):
        dep_value, lat_t, lon_t, shift_value = inputs
        row_block = lax.dynamic_slice_in_dim(fields, (dep_value - 1).astype(jnp.int32), 4, 0)
        lat_w = cubic_weights(lat_t)
        column = lat_w[0] * row_block[0] + lat_w[1] * row_block[1] + lat_w[2] * row_block[2] + lat_w[3] * row_block[3]
        return along_lon(column, cubic_weights(lon_t), shift_value)

    moved = lax.map(one_row, (departure, lat_fraction, lon_fraction, lon_shift))
    area = jnp.cos(math.pi * (row_ids.astype(jnp.float32) + 0.5) / NLAT - math.pi / 2.0)
    mass_before = jnp.sum(area[:, None, None, None] * fields, axis=(0, 2, 3))
    mass_after = jnp.sum(area[:, None, None, None] * moved, axis=(0, 2, 3))
    return moved * (mass_before / mass_after)[None, :, None, None]
```

```python
import functools
import math

import jax
import jax.numpy as jnp
import numpy as np
from jax import lax
from jax.experimental import pallas as pl
from jax.experimental.pallas import tpu as pltpu
from jax.sharding import PartitionSpec as P

GROUP = 4
LANES = 128
PARTS = 5
LEAD = 4
LAG = 2
MESH = pl.DeviceIdType.MESH


def cubic(t):
    sixth = 1.0 / 6.0
    return (
        -t * (t - 1.0) * (t - 2.0) * sixth,
        (t + 1.0) * (t - 1.0) * (t - 2.0) * 0.5,
        -(t + 1.0) * t * (t - 2.0) * 0.5,
        (t + 1.0) * t * (t - 1.0) * sixth,
    )


def departure_of(departure, north, south, first_row, rows, total_rows):
    low = first_row - north * rows + 1
    high = first_row + rows - 3 + south * rows
    inside = jnp.minimum(jnp.maximum(departure, low), high)
    return jnp.minimum(jnp.maximum(inside, 1), total_rows - 3)


def chunks_of(field_count, lon_count):
    tiles = lon_count // (GROUP * LANES)
    parts = min(PARTS, tiles)
    edges = [tiles * n // parts for n in range(parts + 1)]
    return [
        (f, edges[n] * LANES, (edges[n + 1] - edges[n]) * LANES) for f in range(field_count) for n in range(parts)
    ]


def exchange_kernel(bands, levs, chunks, lat_t_ref, lon_t_ref, departure_ref, extents_ref, area_ref, fields_ref,
                    column_ref, table_ref, held, far_departure, far_extents, far_lat, start_of, weight_of, mine, met,
                    sent, gathered, load_sem, note_send, note_recv, give_send, give_recv, pass_send, pass_recv,
                    slice_sem, bring_send, bring_recv, keep_sem, table_send_sem, table_recv_sem, *buffers):
    band, lev = lax.axis_index("lat"), lax.axis_index("lev")
    group, position = band // GROUP, lax.rem(band, GROUP)
    groups = bands // GROUP
    has_up = group < groups - 1
    has_down = group > 0
    rows, field_count, _, lon_count = fields_ref.shape
    width = lon_count // GROUP
    count = len(chunks)
    source, mixed = buffers[:count], buffers[count:]
    first_row, total_rows = band * rows, bands * rows
    step_one = 1 - 2 * lax.rem(position, 2)
    step_two = 2 - 4 * (position // 2)
    steps = [step_one, step_two, step_one + step_two]
    across = [{"lev": 1 - lev}, {"lat": band + step_one}, {"lat": band + step_two}]
    others = [{"lat": lax.rem(band + GROUP * j, bands)} for j in range(1, groups)]

    load = pltpu.make_async_copy(fields_ref, held, load_sem)
    load.start()

    barrier = pltpu.get_barrier_semaphore()
    greeted = across + [{"lat": band + steps[2]}] + others
    for peer in greeted:
        pl.semaphore_signal(barrier, inc=1, device_id=peer, device_id_type=MESH)
    pl.semaphore_wait(barrier, len(greeted))

    def remote(source_ref, target_ref, send_sem, recv_sem, peer):
        return pltpu.make_async_remote_copy(
            src_ref=source_ref, dst_ref=target_ref, send_sem=send_sem, recv_sem=recv_sem,
            device_id=peer, device_id_type=MESH,
        )

    def slice_at(home, k):
        first, size = chunks[k][1:]
        return pl.ds(pl.multiple_of(home * width + first, LANES), size)

    def fields_cut(home, k):
        return fields_ref.at[:, chunks[k][0], :, slice_at(home, k)]

    def source_cut(k, n):
        return source[k].at[pl.ds(n * rows, rows)]

    def note(n, j):
        here, there = ((departure_ref, far_departure), (extents_ref.at[0], far_extents), (lat_t_ref, far_lat))[n]
        return remote(here, there.at[position], note_send.at[n, j], note_recv.at[n, j], {"lat": band + steps[j]})

    def give(j, k):
        home = position + steps[j]
        return remote(
            fields_cut(home, k), source_cut(k, GROUP + position), give_send.at[j], give_recv.at[j, k],
            {"lat": band + steps[j]},
        )

    def own_slice(k):
        return pltpu.make_async_copy(fields_cut(position, k), source_cut(k, GROUP + position), slice_sem.at[k])

    def pass_on(k, member, block):
        up = remote(
            block, source_cut(k, member), pass_send.at[0], pass_recv.at[0, k], {"lat": band + GROUP}
        )
        down = remote(
            block, source_cut(k, 2 * GROUP + member), pass_send.at[1], pass_recv.at[1, k], {"lat": band - GROUP}
        )
        pl.when(has_up)(up.start)
        pl.when(has_down)(down.start)

    def bring(j, k):
        return remote(
            mixed[k].at[pl.ds((position + steps[j]) * rows, rows)],
            column_ref.at[:, chunks[k][0], :, slice_at(position, k)],
            bring_send.at[j], bring_recv.at[j, k], {"lat": band + steps[j]},
        )

    def keep(k):
        return pltpu.make_async_copy(
            mixed[k].at[pl.ds(position * rows, rows)],
            column_ref.at[:, chunks[k][0], :, slice_at(position, k)], keep_sem.at[k],
        )

    def table_copy(n, block, target, peer):
        return remote(block, target, table_send_sem.at[n], table_recv_sem.at[n], peer)

    def table_step(n):
        return table_copy(n, mine if n == 0 else sent.at[n - 1], met.at[n], across[n])

    def table_add(n):
        table_step(n).wait_recv()
        sent[n] = (mine[...] if n == 0 else sent[n - 1]) + met[n]

    last = [table_copy(3 + j, sent.at[2], gathered.at[j], peer) for j, peer in enumerate(others)]

    def pass_own(k):
        if k < count:
            pass_on(k, position, fields_cut(position, k))

    def take(k):
        for j in range(3):
            give(j, k).wait_recv()
            member = position + steps[j]
            pass_on(k, member, source_cut(k, GROUP + member))
        pass_own(k + LEAD)

    def combine(k):
        own_slice(k).wait()

        @pl.when(has_down)
        def _():
            block = source[k].at[pl.ds(0, GROUP * rows)]
            remote(block, block, pass_send.at[0], pass_recv.at[0, k], {"lat": band}).wait_recv()

        @pl.when(has_up)
        def _():
            block = source[k].at[pl.ds(2 * GROUP * rows, GROUP * rows)]
            remote(block, block, pass_send.at[1], pass_recv.at[1, k], {"lat": band}).wait_recv()

        def one_row(n, carry):
            first = start_of[n]
            weights = [weight_of[GROUP * n + a] for a in range(4)]
            for t in range(chunks[k][2] // LANES):
                at = pl.ds(t * LANES, LANES)
                total = weights[0] * source[k][first, :, at]
                for a in range(1, 4):
                    total = total + weights[a] * source[k][first + a, :, at]
                mixed[k][n, :, at] = total
            return carry

        lax.fori_loop(0, GROUP * rows, one_row, 0, unroll=4)
        for j in range(3):
            bring(j, k).start()
        keep(k).start()

    for n in range(3):
        for j in range(3):
            note(n, j).start()
    for k in range(count):
        for j in range(3):
            give(j, k).start()
        if k < LEAD:
            pass_own(k)
    for k in range(count):
        own_slice(k).start()

    lane = lax.broadcasted_iota(jnp.int32, (1, table_ref.shape[1]), 1)
    taken = jnp.zeros(lane.shape, jnp.float32)
    for row in range(rows):
        departure = departure_of(
            departure_ref[row], extents_ref[0, 0], extents_ref[0, 1], first_row, rows, total_rows
        )
        lon_w = cubic(lon_t_ref[row])
        share = area_ref[first_row + row] * (lon_w[0] + lon_w[1] + lon_w[2] + lon_w[3]) * (1.0 / levs)
        for a, weight in enumerate(cubic(lat_t_ref[row])):
            taken = taken + jnp.where(lane == departure - 1 + a, share * weight, 0.0)
    load.wait()
    sums = [jnp.zeros(lane.shape, jnp.float32) for _ in range(field_count)]
    for row in range(rows):
        for f in range(field_count):
            total = jnp.sum(jnp.sum(held[row, f], axis=0, keepdims=True), axis=1, keepdims=True)
            sums[f] = sums[f] + jnp.where(lane == first_row + row, total, 0.0)
    mine[...] = jnp.zeros_like(mine)
    for f in range(field_count):
        mine[f:f + 1, :] = sums[f]
    mine[field_count:field_count + 1, :] = taken
    table_step(0).start()

    take(0)
    for row in range(rows):
        far_departure[position, row] = departure_ref[row]
        far_lat[position, row] = lat_t_ref[row]
    for e in range(2):
        far_extents[position, e] = extents_ref[0, e]
    for n in range(3):
        for j in range(3):
            note(n, j).wait_recv()
    for member in range(GROUP):
        member_row = (group * GROUP + member) * rows
        north, south = far_extents[member, 0], far_extents[member, 1]

        def prepare(row, carry):
            departure = departure_of(far_departure[member, row], north, south, member_row, rows, total_rows)
            start_of[member * rows + row] = departure - 1 - (group - 1) * GROUP * rows
            for a, weight in enumerate(cubic(far_lat[member, row])):
                weight_of[GROUP * (member * rows + row) + a] = weight
            return carry

        lax.fori_loop(0, rows, prepare, 0)

    table_add(0)
    table_step(1).start()
    done = 0
    for k in range(1, count):
        take(k)
        while done < count and 2 * done + 1 + LAG <= k:
            combine(done)
            done += 1
        if k == count // 3:
            table_add(1)
            table_step(2).start()
        if k == count - 1:
            table_add(2)
            for copy in last:
                copy.start()
    while done < count:
        combine(done)
        done += 1

    for copy in last:
        copy.wait_recv()
    result = sent[2]
    for j in range(len(others)):
        result = result + gathered[j]
    table_ref[...] = result

    for k in range(count):
        for j in range(3):
            home = position + steps[j]
            block = column_ref.at[:, chunks[k][0], :, slice_at(home, k)]
            remote(block, block, bring_send.at[j], bring_recv.at[j, k], {"lat": band}).wait_recv()
        keep(k).wait()
    for k in range(count):
        for j in range(3):
            give(j, k).wait_send()
            bring(j, k).wait_send()
        for _ in range(GROUP):
            @pl.when(has_up)
            def _():
                remote(
                    source_cut(k, 0), source_cut(k, 0), pass_send.at[0], pass_recv.at[0, k], {"lat": band}
                ).wait_send()

            @pl.when(has_down)
            def _():
                remote(
                    source_cut(k, 0), source_cut(k, 0), pass_send.at[1], pass_recv.at[1, k], {"lat": band}
                ).wait_send()
    for n in range(3):
        for j in range(3):
            note(n, j).wait_send()
        table_step(n).wait_send()
    for copy in last:
        copy.wait_send()


def exchange(lat_t, lon_t, departure_row, extents, area, fields):
    bands, levs = lax.axis_size("lat"), lax.axis_size("lev")
    rows, field_count, levels, lon_count = fields.shape
    table = ((field_count + 8) // 8 * 8, -(-bands * rows // LANES) * LANES)
    others = bands // GROUP - 1
    chunks = chunks_of(field_count, lon_count)
    count = len(chunks)
    dma = pltpu.SemaphoreType.DMA
    return pl.pallas_call(
        functools.partial(exchange_kernel, bands, levs, chunks),
        out_shape=(
            jax.ShapeDtypeStruct(fields.shape, fields.dtype),
            jax.ShapeDtypeStruct(table, jnp.float32),
        ),
        in_specs=[pl.BlockSpec(memory_space=pltpu.SMEM)] * 5 + [pl.BlockSpec(memory_space=pl.ANY)],
        out_specs=(pl.BlockSpec(memory_space=pl.ANY), pl.BlockSpec(memory_space=pltpu.VMEM)),
        scratch_shapes=[
            pltpu.VMEM(fields.shape, jnp.float32),
            pltpu.SMEM((GROUP, rows), jnp.int32),
            pltpu.SMEM((GROUP, 2), jnp.int32),
            pltpu.SMEM((GROUP, rows), jnp.float32),
            pltpu.SMEM((GROUP * rows,), jnp.int32),
            pltpu.SMEM((4 * GROUP * rows,), jnp.float32),
            pltpu.VMEM(table, jnp.float32),
            pltpu.VMEM((3,) + table, jnp.float32),
            pltpu.VMEM((3,) + table, jnp.float32),
            pltpu.VMEM((max(others, 1),) + table, jnp.float32),
            dma,
            dma((3, 3)),
            dma((3, 3)),
            dma((3,)),
            dma((3, count)),
            dma((2,)),
            dma((2, count)),
            dma((count,)),
            dma((3,)),
            dma((3, count)),
            dma((count,)),
            dma((3 + others,)),
            dma((3 + others,)),
        ]
        + [pltpu.VMEM((3 * GROUP * rows, levels, size), jnp.float32) for _, _, size in chunks]
        + [pltpu.VMEM((GROUP * rows, levels, size), jnp.float32) for _, _, size in chunks],
        compiler_params=pltpu.CompilerParams(collective_id=0, has_side_effects=True),
        name="exchange",
    )(lat_t, lon_t, departure_row, extents, area, fields)


def row_kernel(lon_t_ref, shift_ref, table_ref, area_ref, column_ref, out_ref, doubled, ratio):
    row = pl.program_id(0)
    _, field_count, _, lon_count = column_ref.shape
    tiles = lon_count // LANES

    @pl.when(row == 0)
    def _():
        weight = table_ref[field_count:field_count + 1, :]
        for f in range(field_count):
            total = table_ref[f:f + 1, :]
            before = jnp.sum(total * area_ref[...], axis=1, keepdims=True)
            after = jnp.sum(total * weight, axis=1, keepdims=True)
            ratio[f] = jnp.broadcast_to(before / after, ratio.shape[1:])

    lon_w = cubic(lon_t_ref[row])
    lane = lax.broadcasted_iota(jnp.int32, (out_ref.shape[2], LANES), 1)
    first = lax.rem(shift_ref[row] - 1 + lon_count, lon_count)
    whole, rest = first // LANES, lax.rem(first, LANES)
    turn = lax.rem(LANES - rest, LANES)
    keep = lane < LANES - rest

    def ahead(pieces, step):
        turned = [pltpu.roll(piece, LANES - step, 1) for piece in pieces]
        return [jnp.where(lane < LANES - step, turned[t], turned[(t + 1) % tiles]) for t in range(tiles)]

    for f in range(field_count):
        lon = [weight * ratio[f] for weight in lon_w]
        column = [column_ref[0, f, :, t * LANES:(t + 1) * LANES] for t in range(tiles)]
        after = ahead(column, 1)
        later = ahead([lon[2] * column[t] + lon[3] * after[t] for t in range(tiles)], 2)
        for t in range(tiles):
            moved = lon[0] * column[t] + lon[1] * after[t] + later[t]
            doubled[f, :, t * LANES:(t + 1) * LANES] = moved
            doubled[f, :, lon_count + t * LANES:lon_count + (t + 1) * LANES] = moved
        turned = []
        for t in range(tiles + 1):
            at = pl.multiple_of((whole + t) * LANES, LANES)
            turned.append(pltpu.roll(doubled[f, :, pl.ds(at, LANES)], turn, 1))
        for t in range(tiles):
            out_ref[0, f, :, t * LANES:(t + 1) * LANES] = jnp.where(keep, turned[t], turned[t + 1])


def rows_of(lon_t, shift, table, area, column):
    rows, field_count, levels, lon_count = column.shape
    smem = pl.BlockSpec(memory_space=pltpu.SMEM)
    vmem = pl.BlockSpec(memory_space=pltpu.VMEM)
    row_block = pl.BlockSpec((1, field_count, levels, lon_count), lambda r: (r, 0, 0, 0))
    return pl.pallas_call(
        row_kernel,
        grid=(rows,),
        out_shape=jax.ShapeDtypeStruct(column.shape, column.dtype),
        in_specs=[smem, smem, vmem, vmem, row_block],
        out_specs=row_block,
        scratch_shapes=[
            pltpu.VMEM((field_count, levels, 2 * lon_count), jnp.float32),
            pltpu.VMEM((field_count, levels, LANES), jnp.float32),
        ],
        compiler_params=pltpu.CompilerParams(dimension_semantics=("arbitrary",)),
        name="rows",
    )(lon_t, shift, table, area, column)


def per_device(fields, lat_fraction, lon_fraction, lon_shift, departure_row, extents):
    bands = lax.axis_size("lat")
    total_rows = bands * fields.shape[0]
    row_ids = np.arange(-(-total_rows // LANES) * LANES)
    area = np.where(row_ids < total_rows, np.cos(math.pi * (row_ids + 0.5) / total_rows - math.pi / 2.0), 0.0)
    area = jnp.asarray(area, jnp.float32)
    column, table = exchange(lat_fraction, lon_fraction, departure_row, extents, area, fields)
    return rows_of(lon_fraction, lon_shift, table, area[None, :], column)


def solution(mesh):
    return jax.shard_map(
        per_device,
        mesh=mesh,
        in_specs=(
            P("lat", None, "lev", None),
            P("lat"),
            P("lat"),
            P("lat"),
            P("lat"),
            P("lat", None),
        ),
        out_specs=P("lat", None, "lev", None),
        check_vma=False,
    )
```

```python
import functools
import math

import jax
import jax.numpy as jnp
import numpy as np
from jax import lax
from jax.experimental import pallas as pl
from jax.experimental.pallas import tpu as pltpu
from jax.sharding import PartitionSpec as P

GROUP = 4
LANES = 128
PARTS = (3, 3, 3)
GIVEN = 4
PASSED = 2
WAIT = 1
VMEM_BYTES = 40 * 1024 * 1024
MESH = pl.DeviceIdType.MESH


def cubic(t):
    sixth = 1.0 / 6.0
    return (
        -t * (t - 1.0) * (t - 2.0) * sixth,
        (t + 1.0) * (t - 1.0) * (t - 2.0) * 0.5,
        -(t + 1.0) * t * (t - 2.0) * 0.5,
        (t + 1.0) * t * (t - 1.0) * sixth,
    )


def departure_of(departure, north, south, first_row, rows, total_rows):
    low = first_row - north * rows + 1
    high = first_row + rows - 3 + south * rows
    inside = jnp.minimum(jnp.maximum(departure, low), high)
    return jnp.minimum(jnp.maximum(inside, 1), total_rows - 3)


def chunks_of(field_count, lon_count):
    tiles = lon_count // (GROUP * LANES)
    chunks = []
    for f in range(field_count):
        parts = min(PARTS[min(f, len(PARTS) - 1)], tiles)
        edges = [tiles * n // parts for n in range(parts + 1)]
        if f == field_count - 1:
            edges = [tiles - edge for edge in reversed(edges)]
        chunks += [(f, low * LANES, (high - low) * LANES) for low, high in zip(edges, edges[1:])]
    return chunks


def advect_kernel(bands, levs, chunks, lat_t_hbm, lon_t_hbm, shift_hbm, departure_hbm, extents_hbm, area_hbm,
                  fields_ref, moved_ref, lat_t_ref, lon_t_ref, shift_ref, departure_ref, extents_ref,
                  area_ref, held, far_departure, far_extents, far_lat, start_of, weight_of, lon_of, mine, met, plane,
                  below, above, upward, downward, ratio, scalar_sem, load_sem, note_send, note_recv, give_send,
                  give_recv, pass_send, pass_recv, slice_sem, bring_send, bring_recv, keep_sem, table_send,
                  table_recv, chain_send, chain_recv, *buffers):
    band, lev = lax.axis_index("lat"), lax.axis_index("lev")
    group, position = band // GROUP, lax.rem(band, GROUP)
    groups = bands // GROUP
    has_up = group < groups - 1
    has_down = group > 0
    rows, field_count, levels, lon_count = fields_ref.shape
    width = lon_count // GROUP
    tiles = lon_count // LANES
    count = len(chunks)
    source, mixed = buffers[:count], buffers[count:2 * count]
    column = buffers[2 * count:]
    first_row, total_rows = band * rows, bands * rows
    step_one = 1 - 2 * lax.rem(position, 2)
    step_two = 2 - 4 * (position // 2)
    steps = [step_one, step_two, step_one + step_two]
    mates = [{"lat": band + step, "lev": (lev + n) % levs} for n in range(levs) for step in [0] + steps][1:]
    up_peer, down_peer = {"lat": band + GROUP}, {"lat": band - GROUP}

    def signal(peer):
        pl.semaphore_signal(barrier, inc=1, device_id=peer, device_id_type=MESH)

    barrier = pltpu.get_barrier_semaphore()
    for peer in mates:
        signal(peer)
    pl.when(has_up)(lambda: signal(up_peer))
    pl.when(has_down)(lambda: signal(down_peer))

    scalars = [
        pltpu.make_async_copy(there, here, scalar_sem.at[n])
        for n, (there, here) in enumerate((
            (departure_hbm, departure_ref), (extents_hbm, extents_ref), (lat_t_hbm, lat_t_ref),
            (lon_t_hbm, lon_t_ref), (shift_hbm, shift_ref), (area_hbm, area_ref),
        ))
    ]
    for copy in scalars:
        copy.start()
    load = pltpu.make_async_copy(fields_ref, held, load_sem)
    load.start()

    pl.semaphore_wait(barrier, len(mates) + has_up.astype(jnp.int32) + has_down.astype(jnp.int32))

    def remote(source_ref, target_ref, send_sem, recv_sem, peer):
        return pltpu.make_async_remote_copy(
            src_ref=source_ref, dst_ref=target_ref, send_sem=send_sem, recv_sem=recv_sem,
            device_id=peer, device_id_type=MESH,
        )

    def slice_at(home, k):
        first, size = chunks[k][1:]
        return pl.ds(pl.multiple_of(home * width + first, LANES), size)

    def fields_cut(home, k):
        return fields_ref.at[:, chunks[k][0], :, slice_at(home, k)]

    def source_cut(k, n, blocks=1):
        return source[k].at[pl.ds(n * rows, blocks * rows)]

    def column_cut(home, k):
        f, first, size = chunks[k]
        return column[f].at[:, pl.ds((home * width + first) // LANES, size // LANES)]

    def note(n, j):
        here, there = ((departure_ref, far_departure), (extents_ref.at[0], far_extents), (lat_t_ref, far_lat))[n]
        return remote(here, there.at[position], note_send.at[n, j], note_recv.at[n, j], {"lat": band + steps[j]})

    def give(j, k):
        home = position + steps[j]
        return remote(
            fields_cut(home, k), source_cut(k, GROUP + position), give_send.at[j], give_recv.at[j, k],
            {"lat": band + steps[j]},
        )

    def own_slice(k):
        return pltpu.make_async_copy(fields_cut(position, k), source_cut(k, GROUP + position), slice_sem.at[k])

    def pass_up(k, block, n, blocks=1):
        return remote(block, source_cut(k, n, blocks), pass_send.at[0], pass_recv.at[0, k], up_peer)

    def pass_down(k, block, n, blocks=1):
        return remote(block, source_cut(k, 2 * GROUP + n, blocks), pass_send.at[1], pass_recv.at[1, k], down_peer)

    def pass_on(k, member, block):
        pl.when(has_up)(pass_up(k, block, member).start)
        pl.when(has_down)(pass_down(k, block, member).start)

    def bring(j, k):
        return remote(
            mixed[k].at[pl.ds((position + steps[j]) * rows, rows)], column_cut(position, k),
            bring_send.at[j], bring_recv.at[j, k], {"lat": band + steps[j]},
        )

    def keep(k):
        return pltpu.make_async_copy(
            mixed[k].at[pl.ds(position * rows, rows)], column_cut(position, k), keep_sem.at[k]
        )

    def table_copy(n):
        return remote(mine, met.at[n], table_send.at[n], table_recv.at[n], mates[n])

    up_copy = remote(upward, below, chain_send.at[0], chain_recv.at[0], up_peer)
    down_copy = remote(downward, above, chain_send.at[1], chain_recv.at[1], down_peer)

    def give_all(k):
        if k < count:
            for j in range(3):
                give(j, k).start()

    def pass_own(k):
        if k < count:
            pass_on(k, position, fields_cut(position, k))

    def take(k):
        if k >= count:
            return
        for j in range(3):
            give(j, k).wait_recv()
            member = position + steps[j]
            pass_on(k, member, source_cut(k, GROUP + member))

    def combine(k):
        own_slice(k).wait()
        pl.when(has_down)(pass_up(k, source_cut(k, 0, GROUP), 0, GROUP).wait_recv)
        pl.when(has_up)(pass_down(k, source_cut(k, 0, GROUP), 0, GROUP).wait_recv)

        def one_row(n, carry):
            first = start_of[n]
            weights = [weight_of[4 * n + a] for a in range(4)]
            for t in range(chunks[k][2] // LANES):
                at = pl.ds(t * LANES, LANES)
                total = weights[0] * source[k][first, :, at]
                for a in range(1, 4):
                    total = total + weights[a] * source[k][first + a, :, at]
                mixed[k][n, t] = total
            return carry

        lax.fori_loop(0, GROUP * rows, one_row, 0, unroll=4)
        for j in range(3):
            bring(j, k).start()
        keep(k).start()

    def chain(hop):
        if hop == 0:
            total = mine[...]
            for n in range(len(mates)):
                table_copy(n).wait_recv()
                total = total + met[n]
            plane[...] = total

            @pl.when(jnp.logical_not(has_down))
            def _():
                below[...] = jnp.zeros_like(below)

            @pl.when(jnp.logical_not(has_up))
            def _():
                above[...] = jnp.zeros_like(above)

        @pl.when(group == hop)
        def _():
            if hop > 0:
                up_copy.wait_recv()
            if hop < groups - 1:
                upward[...] = plane[...] + below[...]
                up_copy.start()

        @pl.when(group == groups - 1 - hop)
        def _():
            if hop > 0:
                down_copy.wait_recv()
            if hop < groups - 1:
                downward[...] = plane[...] + above[...]
                down_copy.start()

    def find_ratio():
        total = plane[...] + below[...] + above[...]
        for f in range(field_count):
            sums_at = total[f:f + 1, :]
            mass_before = jnp.sum(sums_at * total[field_count + 1:field_count + 2, :], axis=1, keepdims=True)
            mass_after = jnp.sum(sums_at * total[field_count:field_count + 1, :], axis=1, keepdims=True)
            ratio[f:f + 1, :] = jnp.broadcast_to(mass_before / mass_after, (1, LANES))

    def along_lon(f):
        for k in range(count):
            if chunks[k][0] == f:
                for j in range(3):
                    block = column_cut(position + steps[j], k)
                    remote(block, block, bring_send.at[j], bring_recv.at[j, k], {"lat": band}).wait_recv()
                keep(k).wait()
        lane = lax.broadcasted_iota(jnp.int32, (levels, LANES), 1)
        scale = jnp.broadcast_to(ratio[f:f + 1, :], (levels, LANES))

        def one_row(row, carry):
            for t in range(tiles):
                column[f][row, tiles + t] = column[f][row, t]
            column[f][row, 2 * tiles] = column[f][row, 0]
            lon = [lon_of[4 * row + n] * scale for n in range(4)]
            first = lax.rem(shift_ref[row] - 1 + lon_count, lon_count)
            rests = [lax.rem(first + n, LANES) for n in range(4)]
            turns = [lax.rem(LANES - rest, LANES) for rest in rests]
            stays = [lane < LANES - rest for rest in rests]
            bases = [(first + n) // LANES for n in range(4)]

            def turned(t):
                return [pltpu.roll(column[f][row, bases[n] + t], turns[n], 1) for n in range(4)]

            here = turned(0)
            for t in range(tiles):
                there = turned(t + 1)
                total = lon[0] * jnp.where(stays[0], here[0], there[0])
                for n in range(1, 4):
                    total = total + lon[n] * jnp.where(stays[n], here[n], there[n])
                moved_ref[row, f, :, pl.ds(t * LANES, LANES)] = total
                here = there
            return carry

        lax.fori_loop(0, rows, one_row, 0)

    pass_own(0)
    give_all(0)
    pass_own(1)
    for copy in scalars:
        copy.wait()
    for n in range(3):
        for j in range(3):
            note(n, j).start()
    load.wait()
    lane = lax.broadcasted_iota(jnp.int32, (1, mine.shape[1]), 1)
    taken = jnp.zeros(lane.shape, jnp.float32)
    for row in range(rows):
        departure = departure_of(
            departure_ref[row], extents_ref[0, 0], extents_ref[0, 1], first_row, rows, total_rows
        )
        lon_w = cubic(lon_t_ref[row])
        for n, weight in enumerate(lon_w):
            lon_of[4 * row + n] = weight
        share = area_ref[first_row + row] * (lon_w[0] + lon_w[1] + lon_w[2] + lon_w[3]) * (1.0 / levs)
        for a, weight in enumerate(cubic(lat_t_ref[row])):
            taken = taken + jnp.where(lane == departure - 1 + a, share * weight, 0.0)
    sums = [jnp.zeros(lane.shape, jnp.float32) for _ in range(field_count)]
    before = jnp.zeros(lane.shape, jnp.float32)
    for row in range(rows):
        before = before + jnp.where(lane == first_row + row, area_ref[first_row + row] * (1.0 / levs), 0.0)
        for f in range(field_count):
            total = jnp.sum(jnp.sum(held[row, f], axis=0, keepdims=True), axis=1, keepdims=True)
            sums[f] = sums[f] + jnp.where(lane == first_row + row, total, 0.0)
    mine[...] = jnp.zeros_like(mine)
    for f in range(field_count):
        mine[f:f + 1, :] = sums[f]
    mine[field_count:field_count + 1, :] = taken
    mine[field_count + 1:field_count + 2, :] = before
    for n in range(len(mates)):
        table_copy(n).start()

    for k in range(1, GIVEN):
        give_all(k)
    for k in range(count):
        own_slice(k).start()
    for k in range(PASSED):
        if k >= 2:
            pass_own(k)
        take(k)
    for row in range(rows):
        far_departure[position, row] = departure_ref[row]
        far_lat[position, row] = lat_t_ref[row]
    for e in range(2):
        far_extents[position, e] = extents_ref[0, e]
    for n in range(3):
        for j in range(3):
            note(n, j).wait_recv()
    for member in range(GROUP):
        member_row = (group * GROUP + member) * rows
        north, south = far_extents[member, 0], far_extents[member, 1]

        def prepare(row, carry):
            departure = departure_of(far_departure[member, row], north, south, member_row, rows, total_rows)
            start_of[member * rows + row] = departure - 1 - (group - 1) * GROUP * rows
            for a, weight in enumerate(cubic(far_lat[member, row])):
                weight_of[4 * (member * rows + row) + a] = weight
            return carry

        lax.fori_loop(0, rows, prepare, 0)
    chain(0)

    hop = 1
    finished = 0
    for k in range(count):
        give_all(k + GIVEN)
        pass_own(k + PASSED)
        take(k + PASSED)
        combine(k)
        while hop < groups and (hop * (count - WAIT)) // groups <= k:
            chain(hop)
            hop += 1
            if hop == groups:
                find_ratio()
        if k < count - 1 and hop == groups and chunks[k - WAIT][0] > finished:
            along_lon(finished)
            finished += 1
    for f in range(finished, field_count):
        along_lon(f)

    for k in range(count):
        for j in range(3):
            give(j, k).wait_send()
            bring(j, k).wait_send()
        pl.when(has_up)(pass_up(k, source_cut(k, 0, GROUP), 0, GROUP).wait_send)
        pl.when(has_down)(pass_down(k, source_cut(k, 0, GROUP), 0, GROUP).wait_send)
    for n in range(3):
        for j in range(3):
            note(n, j).wait_send()
    for n in range(len(mates)):
        table_copy(n).wait_send()
    pl.when(has_up)(up_copy.wait_send)
    pl.when(has_down)(down_copy.wait_send)


def advect(lat_t, lon_t, shift, departure_row, extents, area, fields):
    bands, levs = lax.axis_size("lat"), lax.axis_size("lev")
    rows, field_count, levels, lon_count = fields.shape
    table = (-(-(field_count + 2) // 8) * 8, -(-bands * rows // LANES) * LANES)
    mates = GROUP * levs - 1
    chunks = chunks_of(field_count, lon_count)
    count = len(chunks)
    dma = pltpu.SemaphoreType.DMA
    hbm = pl.BlockSpec(memory_space=pltpu.HBM)
    operands = (lat_t, lon_t, shift, departure_row, extents, area, fields)
    return pl.pallas_call(
        functools.partial(advect_kernel, bands, levs, chunks),
        out_shape=jax.ShapeDtypeStruct(fields.shape, fields.dtype),
        in_specs=[hbm] * 7,
        out_specs=pl.BlockSpec(memory_space=pltpu.VMEM),
        scratch_shapes=[
            pltpu.SMEM(lat_t.shape, jnp.float32),
            pltpu.SMEM(lon_t.shape, jnp.float32),
            pltpu.SMEM(shift.shape, jnp.int32),
            pltpu.SMEM(departure_row.shape, jnp.int32),
            pltpu.SMEM(extents.shape, jnp.int32),
            pltpu.SMEM(area.shape, jnp.float32),
            pltpu.VMEM(fields.shape, jnp.float32),
            pltpu.SMEM((GROUP, rows), jnp.int32),
            pltpu.SMEM((GROUP, 2), jnp.int32),
            pltpu.SMEM((GROUP, rows), jnp.float32),
            pltpu.SMEM((GROUP * rows,), jnp.int32),
            pltpu.SMEM((4 * GROUP * rows,), jnp.float32),
            pltpu.SMEM((4 * rows,), jnp.float32),
            pltpu.VMEM(table, jnp.float32),
            pltpu.VMEM((mates,) + table, jnp.float32),
        ]
        + [pltpu.VMEM(table, jnp.float32)] * 5
        + [
            pltpu.VMEM((table[0], LANES), jnp.float32),
            dma((6,)),
            dma,
            dma((3, 3)),
            dma((3, 3)),
            dma((3,)),
            dma((3, count)),
            dma((2,)),
            dma((2, count)),
            dma((count,)),
            dma((3,)),
            dma((3, count)),
            dma((count,)),
            dma((mates,)),
            dma((mates,)),
            dma((2,)),
            dma((2,)),
        ]
        + [pltpu.VMEM((3 * GROUP * rows, levels, size), jnp.float32) for _, _, size in chunks]
        + [pltpu.VMEM((GROUP * rows, size // LANES, levels, LANES), jnp.float32) for _, _, size in chunks]
        + [pltpu.VMEM((rows, 2 * lon_count // LANES + 1, levels, LANES), jnp.float32)] * field_count,
        compiler_params=pltpu.CompilerParams(
            collective_id=0, has_side_effects=True, vmem_limit_bytes=VMEM_BYTES
        ),
        name="advect",
    )(*[pltpu.with_memory_space_constraint(x, pltpu.HBM) for x in operands])


def per_device(fields, lat_fraction, lon_fraction, lon_shift, departure_row, extents):
    bands = lax.axis_size("lat")
    total_rows = bands * fields.shape[0]
    row_ids = np.arange(-(-total_rows // LANES) * LANES)
    area = np.where(row_ids < total_rows, np.cos(math.pi * (row_ids + 0.5) / total_rows - math.pi / 2.0), 0.0)
    area = jnp.asarray(area, jnp.float32)
    return advect(lat_fraction, lon_fraction, lon_shift, departure_row, extents, area, fields)


def solution(mesh):
    return jax.shard_map(
        per_device,
        mesh=mesh,
        in_specs=(
            P("lat", None, "lev", None),
            P("lat"),
            P("lat"),
            P("lat"),
            P("lat"),
            P("lat", None),
        ),
        out_specs=P("lat", None, "lev", None),
        check_vma=False,
    )
```

```python
import functools
import math

import jax
import jax.numpy as jnp
import numpy as np
from jax import lax
from jax.experimental import pallas as pl
from jax.experimental.pallas import tpu as pltpu
from jax.sharding import PartitionSpec as P

GROUP = 4
LANES = 128
PARTS = (3, 3, 3)
TAIL = 4
GIVEN = 4
PASSED = 2
WAIT = 1
ROLL = 5
OWN = 3
VMEM_BYTES = 40 * 1024 * 1024
MESH = pl.DeviceIdType.MESH


def cubic(t):
    sixth = 1.0 / 6.0
    return (
        -t * (t - 1.0) * (t - 2.0) * sixth,
        (t + 1.0) * (t - 1.0) * (t - 2.0) * 0.5,
        -(t + 1.0) * t * (t - 2.0) * 0.5,
        (t + 1.0) * t * (t - 1.0) * sixth,
    )


def departure_of(departure, north, south, first_row, rows, total_rows):
    low = first_row - north * rows + 1
    high = first_row + rows - 3 + south * rows
    inside = jnp.minimum(jnp.maximum(departure, low), high)
    return jnp.minimum(jnp.maximum(inside, 1), total_rows - 3)


def tail_of(lon_count):
    tiles = lon_count // LANES
    return TAIL + (tiles - TAIL) % GROUP


def chunks_of(field_count, lon_count):
    chunks = []
    for f in range(field_count):
        last = f == field_count - 1
        tiles = (lon_count // LANES - (tail_of(lon_count) if last else 0)) // GROUP
        parts = min(PARTS[min(f, len(PARTS) - 1)], tiles)
        edges = [tiles * n // parts for n in range(parts + 1)]
        if last:
            edges = [tiles - edge for edge in reversed(edges)]
        chunks += [(f, low * LANES, (high - low) * LANES) for low, high in zip(edges, edges[1:])]
    return chunks


def advect_kernel(bands, levs, chunks, lat_t_hbm, lon_t_hbm, shift_hbm, departure_hbm, extents_hbm, area_hbm,
                  fields_ref, moved_ref, lat_t_ref, lon_t_ref, shift_ref, departure_ref, extents_ref,
                  area_ref, held, far_departure, far_extents, far_lat, start_of, weight_of, lon_of, mine, pair, met, plane,
                  below, above, upward, downward, ratio, scalar_sem, load_sem, note_send, note_recv, give_send,
                  give_recv, pass_send, pass_recv, slice_sem, bring_send, bring_recv, keep_sem, table_send,
                  table_recv, chain_send, chain_recv, ready_sem,
                  tail_at, tail_weight, tail_raw, tail_own, tail_up, tail_down, tail_below, tail_above, tail_give_send,
                  tail_give_recv, tail_slice_sem, tail_send, tail_recv, *buffers):
    band, lev = lax.axis_index("lat"), lax.axis_index("lev")
    group, position = band // GROUP, lax.rem(band, GROUP)
    groups = bands // GROUP
    has_up = group < groups - 1
    has_down = group > 0
    rows, field_count, levels, lon_count = fields_ref.shape
    tiles = lon_count // LANES
    tail = tail_of(lon_count)
    last_field = field_count - 1
    count = len(chunks)
    source, mixed = buffers[:count], buffers[count:2 * count]
    column = buffers[2 * count:]
    first_row, total_rows = band * rows, bands * rows
    step_one = 1 - 2 * lax.rem(position, 2)
    step_two = 2 - 4 * (position // 2)
    steps = [step_one, step_two, step_one + step_two]
    partner = {"lev": 1 - lev}
    mates = [{"lat": band + step} for step in steps]
    up_peer, down_peer = {"lat": band + GROUP}, {"lat": band - GROUP}

    def signal(peer):
        pl.semaphore_signal(barrier, inc=1, device_id=peer, device_id_type=MESH)

    barrier = pltpu.get_barrier_semaphore()
    for peer in [partner] + mates[:2]:
        signal(peer)
    pl.when(has_up)(lambda: signal(up_peer))
    pl.when(has_down)(lambda: signal(down_peer))

    scalars = [
        pltpu.make_async_copy(there, here, scalar_sem.at[n])
        for n, (there, here) in enumerate((
            (departure_hbm, departure_ref), (extents_hbm, extents_ref), (lat_t_hbm, lat_t_ref),
            (lon_t_hbm, lon_t_ref), (shift_hbm, shift_ref), (area_hbm, area_ref),
        ))
    ]
    for copy in scalars:
        copy.start()
    load = pltpu.make_async_copy(fields_ref, held, load_sem)
    load.start()

    pl.semaphore_wait(barrier, 3 + has_up.astype(jnp.int32) + has_down.astype(jnp.int32))

    def remote(source_ref, target_ref, send_sem, recv_sem, peer):
        return pltpu.make_async_remote_copy(
            src_ref=source_ref, dst_ref=target_ref, send_sem=send_sem, recv_sem=recv_sem,
            device_id=peer, device_id_type=MESH,
        )

    def width_of(f):
        return (lon_count - (tail * LANES if f == last_field else 0)) // GROUP

    def slice_at(home, k):
        f, first, size = chunks[k]
        width = width_of(f)
        return pl.ds(pl.multiple_of(home * width + first, LANES), size)

    def fields_cut(home, k):
        return fields_ref.at[:, chunks[k][0], :, slice_at(home, k)]

    def source_cut(k, n, blocks=1):
        return source[k].at[pl.ds(n * rows, blocks * rows)]

    def column_cut(home, k):
        f, first, size = chunks[k]
        return column[f].at[:, pl.ds((home * width_of(f) + first) // LANES, size // LANES)]

    def note(n, j):
        here, there = ((departure_ref, far_departure), (extents_ref.at[0], far_extents), (lat_t_ref, far_lat))[n]
        slot, peer = ([(position, mate) for mate in mates] + [(GROUP, up_peer), (GROUP + 1, down_peer)])[j]
        return remote(here, there.at[slot], note_send.at[n, j], note_recv.at[n, j], peer)

    def notes(j, act):
        for n in range(3):
            when_z(j - 3, getattr(note(n, j), act))

    def when_z(j, body):
        if j < 0:
            body()
        else:
            pl.when((has_up, has_down)[j])(body)

    def tail_cut():
        return fields_ref.at[:, last_field, :, pl.ds((tiles - tail) * LANES, tail * LANES)]

    def tail_block():
        return tail_raw.at[pl.ds(position * rows, rows)]

    def tail_give(j):
        return remote(tail_cut(), tail_block(), tail_give_send.at[j], tail_give_recv.at[j], mates[j])

    tail_slice = pltpu.make_async_copy(tail_cut(), tail_block(), tail_slice_sem)
    tail_up_copy = remote(tail_up, tail_below, tail_send.at[0], tail_recv.at[0], up_peer)
    tail_down_copy = remote(tail_down, tail_above, tail_send.at[1], tail_recv.at[1], down_peer)

    def give(j, k):
        home = position + steps[j]
        return remote(
            fields_cut(home, k), source_cut(k, GROUP + position), give_send.at[j], give_recv.at[j, k],
            {"lat": band + steps[j]},
        )

    def own_slice(k):
        return pltpu.make_async_copy(fields_cut(position, k), source_cut(k, GROUP + position), slice_sem.at[k])

    def pass_up(k, block, n, blocks=1):
        return remote(block, source_cut(k, n, blocks), pass_send.at[0], pass_recv.at[0, k], up_peer)

    def pass_down(k, block, n, blocks=1):
        return remote(block, source_cut(k, 2 * GROUP + n, blocks), pass_send.at[1], pass_recv.at[1, k], down_peer)

    def pass_on(k, member, block):
        pl.when(has_up)(pass_up(k, block, member).start)
        pl.when(has_down)(pass_down(k, block, member).start)

    def bring(j, k):
        return remote(
            mixed[k].at[pl.ds((position + steps[j]) * rows, rows)], column_cut(position, k),
            bring_send.at[j], bring_recv.at[j, k], {"lat": band + steps[j]},
        )

    def keep(k):
        return pltpu.make_async_copy(
            mixed[k].at[pl.ds(position * rows, rows)], column_cut(position, k), keep_sem.at[k]
        )

    def table_copy(n):
        if n == 0:
            return remote(mine, met.at[0], table_send.at[0], table_recv.at[0], partner)
        return remote(pair, met.at[n], table_send.at[n], table_recv.at[n], mates[n - 1])

    up_copy = remote(upward, below, chain_send.at[0], chain_recv.at[0], up_peer)
    down_copy = remote(downward, above, chain_send.at[1], chain_recv.at[1], down_peer)

    def give_all(k):
        if k <= count:
            for j in range(3):
                (give(j, k) if k < count else tail_give(j)).start()

    def pass_own(k):
        if k < count:
            pass_on(k, position, fields_cut(position, k))

    def take(k):
        if k >= count:
            if k == count:
                tail_combine()
            return
        for j in range(3):
            give(j, k).wait_recv()
            member = position + steps[j]
            pass_on(k, member, source_cut(k, GROUP + member))

    def tail_prepare(n, slot, member_row):
        north, south = far_extents[slot, 0], far_extents[slot, 1]

        def prepare(row, carry):
            departure = departure_of(far_departure[slot, row], north, south, member_row, rows, total_rows)
            for a, weight in enumerate(cubic(far_lat[slot, row])):
                place = departure - 1 + a - group * GROUP * rows
                inside = jnp.logical_and(place >= 0, place < GROUP * rows)
                tail_at[4 * (n * rows + row) + a] = jnp.where(inside, place, 0)
                tail_weight[4 * (n * rows + row) + a] = jnp.where(inside, weight, 0.0)
            return carry

        lax.fori_loop(0, rows, prepare, 0)

    def tail_mix(n, target):
        def one_row(row, carry):
            places = [tail_at[4 * (n * rows + row) + a] for a in range(4)]
            weights = [tail_weight[4 * (n * rows + row) + a] for a in range(4)]
            for t in range(tail):
                at = pl.ds(t * LANES, LANES)
                total = weights[0] * tail_raw[places[0], :, at]
                for a in range(1, 4):
                    total = total + weights[a] * tail_raw[places[a], :, at]
                target[row, t] = total
            return carry

        lax.fori_loop(0, rows, one_row, 0, unroll=2)

    def tail_combine():
        for j in range(3):
            tail_give(j).wait_recv()
        tail_slice.wait()

        @pl.when(has_up)
        def _():
            tail_mix(2, tail_up)
            tail_up_copy.start()

        @pl.when(has_down)
        def _():
            tail_mix(1, tail_down)
            tail_down_copy.start()

        tail_mix(0, tail_own)

        @pl.when(jnp.logical_not(has_down))
        def _():
            tail_below[...] = jnp.zeros_like(tail_below)

        @pl.when(jnp.logical_not(has_up))
        def _():
            tail_above[...] = jnp.zeros_like(tail_above)

    def tail_add():
        pl.when(has_down)(tail_up_copy.wait_recv)
        pl.when(has_up)(tail_down_copy.wait_recv)

        def one_row(row, carry):
            for t in range(tail):
                column[last_field][row, tiles - tail + t] = tail_own[row, t] + tail_below[row, t] + tail_above[row, t]
            return carry

        lax.fori_loop(0, rows, one_row, 0, unroll=2)

    def combine(k):
        own_slice(k).wait()
        pl.when(has_down)(pass_up(k, source_cut(k, 0, GROUP), 0, GROUP).wait_recv)
        pl.when(has_up)(pass_down(k, source_cut(k, 0, GROUP), 0, GROUP).wait_recv)

        def one_row(n, carry):
            first = start_of[n]
            weights = [weight_of[4 * n + a] for a in range(4)]
            for t in range(chunks[k][2] // LANES):
                at = pl.ds(t * LANES, LANES)
                total = weights[0] * source[k][first, :, at]
                for a in range(1, 4):
                    total = total + weights[a] * source[k][first + a, :, at]
                mixed[k][n, t] = total
            return carry

        lax.fori_loop(0, GROUP * rows, one_row, 0, unroll=4)
        for j in range(3):
            bring(j, k).start()
        keep(k).start()

    def chain(hop):
        if hop == 0:
            total = pair[...]
            for n in range(1, 4):
                table_copy(n).wait_recv()
                total = total + met[n]
            plane[...] = total

            @pl.when(jnp.logical_not(has_down))
            def _():
                below[...] = jnp.zeros_like(below)

            @pl.when(jnp.logical_not(has_up))
            def _():
                above[...] = jnp.zeros_like(above)

        @pl.when(group == hop)
        def _():
            if hop > 0:
                up_copy.wait_recv()
            if hop < groups - 1:
                upward[...] = plane[...] + below[...]
                up_copy.start()

        @pl.when(group == groups - 1 - hop)
        def _():
            if hop > 0:
                down_copy.wait_recv()
            if hop < groups - 1:
                downward[...] = plane[...] + above[...]
                down_copy.start()

    def find_ratio():
        total = plane[...] + below[...] + above[...]
        for f in range(field_count):
            sums_at = total[f:f + 1, :]
            mass_before = jnp.sum(sums_at * total[field_count + 1:field_count + 2, :], axis=1, keepdims=True)
            mass_after = jnp.sum(sums_at * total[field_count:field_count + 1, :], axis=1, keepdims=True)
            ratio[f:f + 1, :] = jnp.broadcast_to(mass_before / mass_after, (1, LANES))

    def along_lon(f):
        for k in range(count):
            if chunks[k][0] == f:
                for j in range(3):
                    block = column_cut(position + steps[j], k)
                    remote(block, block, bring_send.at[j], bring_recv.at[j, k], {"lat": band}).wait_recv()
                keep(k).wait()
        if f == last_field:
            tail_add()
        lane = lax.broadcasted_iota(jnp.int32, (levels, LANES), 1)
        scale = jnp.broadcast_to(ratio[f:f + 1, :], (levels, LANES))

        def one_row(row, carry):
            for t in range(tiles):
                column[f][row, tiles + t] = column[f][row, t]
            column[f][row, 2 * tiles] = column[f][row, 0]
            lon = [lon_of[4 * row + n] * scale for n in range(4)]
            first = lax.rem(shift_ref[row] - 1 + lon_count, lon_count)
            rests = [lax.rem(first + n, LANES) for n in range(4)]
            turns = [lax.rem(LANES - rest, LANES) for rest in rests]
            stays = [lane < LANES - rest for rest in rests]
            bases = [(first + n) // LANES for n in range(4)]

            def turned(t):
                return [pltpu.roll(column[f][row, bases[n] + t], turns[n], 1) for n in range(4)]

            here = turned(0)
            for t in range(tiles):
                there = turned(t + 1)
                total = lon[0] * jnp.where(stays[0], here[0], there[0])
                for n in range(1, 4):
                    total = total + lon[n] * jnp.where(stays[n], here[n], there[n])
                moved_ref[row, f, :, pl.ds(t * LANES, LANES)] = total
                here = there
            return carry

        lax.fori_loop(0, rows, one_row, 0, unroll=ROLL)

    pl.semaphore_signal(ready_sem, inc=1, device_id=mates[0], device_id_type=MESH)
    pass_own(0)
    for j in range(2):
        give(j, 0).start()
    for k in range(1, OWN):
        pass_own(k)
    pl.semaphore_wait(ready_sem, 1)
    give(2, 0).start()
    for copy in scalars:
        copy.wait()
    for j in range(5):
        notes(j, "start")
    give_all(1)
    load.wait()
    lane = lax.broadcasted_iota(jnp.int32, (1, mine.shape[1]), 1)
    taken = jnp.zeros(lane.shape, jnp.float32)
    for row in range(rows):
        departure = departure_of(
            departure_ref[row], extents_ref[0, 0], extents_ref[0, 1], first_row, rows, total_rows
        )
        lon_w = cubic(lon_t_ref[row])
        for n, weight in enumerate(lon_w):
            lon_of[4 * row + n] = weight
        share = area_ref[first_row + row] * (lon_w[0] + lon_w[1] + lon_w[2] + lon_w[3]) * (1.0 / levs)
        for a, weight in enumerate(cubic(lat_t_ref[row])):
            taken = taken + jnp.where(lane == departure - 1 + a, share * weight, 0.0)
    sums = [jnp.zeros(lane.shape, jnp.float32) for _ in range(field_count)]
    before = jnp.zeros(lane.shape, jnp.float32)
    for row in range(rows):
        before = before + jnp.where(lane == first_row + row, area_ref[first_row + row] * (1.0 / levs), 0.0)
        for f in range(field_count):
            total = jnp.sum(jnp.sum(held[row, f], axis=0, keepdims=True), axis=1, keepdims=True)
            sums[f] = sums[f] + jnp.where(lane == first_row + row, total, 0.0)
    mine[...] = jnp.zeros_like(mine)
    for f in range(field_count):
        mine[f:f + 1, :] = sums[f]
    mine[field_count:field_count + 1, :] = taken
    mine[field_count + 1:field_count + 2, :] = before
    table_copy(0).start()
    for k in range(count):
        own_slice(k).start()
    tail_slice.start()
    table_copy(0).wait_recv()
    pair[...] = mine[...] + met[0]
    for n in range(1, 4):
        table_copy(n).start()
    for k in range(2, GIVEN):
        give_all(k)
    for k in range(PASSED):
        take(k)
    for row in range(rows):
        far_departure[position, row] = departure_ref[row]
        far_lat[position, row] = lat_t_ref[row]
    for e in range(2):
        far_extents[position, e] = extents_ref[0, e]
    for n in range(3):
        for j in range(3):
            note(n, j).wait_recv()
        pl.when(has_down)(note(n, 3).wait_recv)
        pl.when(has_up)(note(n, 4).wait_recv)
    for member in range(GROUP):
        member_row = (group * GROUP + member) * rows
        north, south = far_extents[member, 0], far_extents[member, 1]

        def prepare(row, carry):
            departure = departure_of(far_departure[member, row], north, south, member_row, rows, total_rows)
            start_of[member * rows + row] = departure - 1 - (group - 1) * GROUP * rows
            for a, weight in enumerate(cubic(far_lat[member, row])):
                weight_of[4 * (member * rows + row) + a] = weight
            return carry

        lax.fori_loop(0, rows, prepare, 0)
    chain(0)
    tail_prepare(0, position, first_row)
    pl.when(has_down)(lambda: tail_prepare(1, GROUP, first_row - GROUP * rows))
    pl.when(has_up)(lambda: tail_prepare(2, GROUP + 1, first_row + GROUP * rows))

    hop = 1
    finished = 0
    for k in range(count):
        give_all(k + GIVEN)
        pass_own(k + OWN)
        take(k + PASSED)
        combine(k)
        while hop < groups and (hop * (count - WAIT)) // groups <= k:
            chain(hop)
            hop += 1
            if hop == groups:
                find_ratio()
        if k < count - 1 and hop == groups and chunks[k - WAIT][0] > finished:
            along_lon(finished)
            finished += 1
    for f in range(finished, field_count):
        along_lon(f)

    for k in range(count):
        for j in range(3):
            give(j, k).wait_send()
            bring(j, k).wait_send()
        pl.when(has_up)(pass_up(k, source_cut(k, 0, GROUP), 0, GROUP).wait_send)
        pl.when(has_down)(pass_down(k, source_cut(k, 0, GROUP), 0, GROUP).wait_send)
    for j in range(5):
        notes(j, "wait_send")
    for n in range(4):
        table_copy(n).wait_send()
    for j in range(3):
        tail_give(j).wait_send()
    pl.when(has_up)(tail_up_copy.wait_send)
    pl.when(has_down)(tail_down_copy.wait_send)
    pl.when(has_up)(up_copy.wait_send)
    pl.when(has_down)(down_copy.wait_send)


def advect(lat_t, lon_t, shift, departure_row, extents, area, fields):
    bands, levs = lax.axis_size("lat"), lax.axis_size("lev")
    rows, field_count, levels, lon_count = fields.shape
    table = (-(-(field_count + 2) // 8) * 8, -(-bands * rows // LANES) * LANES)
    tail = tail_of(lon_count)
    tail_block = pltpu.VMEM((rows, tail, levels, LANES), jnp.float32)
    chunks = chunks_of(field_count, lon_count)
    count = len(chunks)
    dma = pltpu.SemaphoreType.DMA
    hbm = pl.BlockSpec(memory_space=pltpu.HBM)
    operands = (lat_t, lon_t, shift, departure_row, extents, area, fields)
    return pl.pallas_call(
        functools.partial(advect_kernel, bands, levs, chunks),
        out_shape=jax.ShapeDtypeStruct(fields.shape, fields.dtype),
        in_specs=[hbm] * 7,
        out_specs=pl.BlockSpec(memory_space=pltpu.VMEM),
        scratch_shapes=[
            pltpu.SMEM(lat_t.shape, jnp.float32),
            pltpu.SMEM(lon_t.shape, jnp.float32),
            pltpu.SMEM(shift.shape, jnp.int32),
            pltpu.SMEM(departure_row.shape, jnp.int32),
            pltpu.SMEM(extents.shape, jnp.int32),
            pltpu.SMEM(area.shape, jnp.float32),
            pltpu.VMEM(fields.shape, jnp.float32),
            pltpu.SMEM((GROUP + 2, rows), jnp.int32),
            pltpu.SMEM((GROUP + 2, 2), jnp.int32),
            pltpu.SMEM((GROUP + 2, rows), jnp.float32),
            pltpu.SMEM((GROUP * rows,), jnp.int32),
            pltpu.SMEM((4 * GROUP * rows,), jnp.float32),
            pltpu.SMEM((4 * rows,), jnp.float32),
            pltpu.VMEM(table, jnp.float32),
            pltpu.VMEM(table, jnp.float32),
            pltpu.VMEM((4,) + table, jnp.float32),
        ]
        + [pltpu.VMEM(table, jnp.float32)] * 5
        + [
            pltpu.VMEM((table[0], LANES), jnp.float32),
            dma((6,)),
            dma,
            dma((3, 5)),
            dma((3, 5)),
            dma((3,)),
            dma((3, count)),
            dma((2,)),
            dma((2, count)),
            dma((count,)),
            dma((3,)),
            dma((3, count)),
            dma((count,)),
            dma((4,)),
            dma((4,)),
            dma((2,)),
            dma((2,)),
            pltpu.SemaphoreType.REGULAR,
            pltpu.SMEM((12 * rows,), jnp.int32),
            pltpu.SMEM((12 * rows,), jnp.float32),
            pltpu.VMEM((GROUP * rows, levels, tail * LANES), jnp.float32),
        ]
        + [tail_block] * 5
        + [
            dma((3,)),
            dma((3,)),
            dma,
            dma((2,)),
            dma((2,)),
        ]
        + [pltpu.VMEM((3 * GROUP * rows, levels, size), jnp.float32) for _, _, size in chunks]
        + [pltpu.VMEM((GROUP * rows, size // LANES, levels, LANES), jnp.float32) for _, _, size in chunks]
        + [pltpu.VMEM((rows, 2 * lon_count // LANES + 1, levels, LANES), jnp.float32)] * field_count,
        compiler_params=pltpu.CompilerParams(
            collective_id=0, has_side_effects=True, vmem_limit_bytes=VMEM_BYTES
        ),
        name="advect",
    )(*[pltpu.with_memory_space_constraint(x, pltpu.HBM) for x in operands])


def per_device(fields, lat_fraction, lon_fraction, lon_shift, departure_row, extents):
    bands = lax.axis_size("lat")
    total_rows = bands * fields.shape[0]
    row_ids = np.arange(-(-total_rows // LANES) * LANES)
    area = np.where(row_ids < total_rows, np.cos(math.pi * (row_ids + 0.5) / total_rows - math.pi / 2.0), 0.0)
    area = jnp.asarray(area, jnp.float32)
    return advect(lat_fraction, lon_fraction, lon_shift, departure_row, extents, area, fields)


def solution(mesh):
    return jax.shard_map(
        per_device,
        mesh=mesh,
        in_specs=(
            P("lat", None, "lev", None),
            P("lat"),
            P("lat"),
            P("lat"),
            P("lat"),
            P("lat", None),
        ),
        out_specs=P("lat", None, "lev", None),
        check_vma=False,
    )
```

```python
import functools
import math

import jax
import jax.numpy as jnp
import numpy as np
from jax import lax
from jax.experimental import pallas as pl
from jax.experimental.pallas import tpu as pltpu
from jax.sharding import PartitionSpec as P

GROUP = 4
LANES = 128
PARTS = (2, 3, 3)
TAIL = 4
GIVEN = 6
PASSED = 3
WAIT = 1
ROLL = 5
OWN = 3
TAIL_GIVE = 0
TAIL_RELAY = 2
VMEM_BYTES = 40 * 1024 * 1024
MESH = pl.DeviceIdType.MESH


def cubic(t):
    sixth = 1.0 / 6.0
    return (
        -t * (t - 1.0) * (t - 2.0) * sixth,
        (t + 1.0) * (t - 1.0) * (t - 2.0) * 0.5,
        -(t + 1.0) * t * (t - 2.0) * 0.5,
        (t + 1.0) * t * (t - 1.0) * sixth,
    )


def departure_of(departure, north, south, first_row, rows, total_rows):
    low = first_row - north * rows + 1
    high = first_row + rows - 3 + south * rows
    inside = jnp.minimum(jnp.maximum(departure, low), high)
    return jnp.minimum(jnp.maximum(inside, 1), total_rows - 3)


def tail_of(lon_count):
    tiles = lon_count // LANES
    return TAIL + (tiles - TAIL) % GROUP


def chunks_of(field_count, lon_count):
    chunks = []
    for f in range(field_count):
        last = f == field_count - 1
        tiles = (lon_count // LANES - (tail_of(lon_count) if last else 0)) // GROUP
        parts = min(PARTS[min(f, len(PARTS) - 1)], tiles)
        edges = [tiles * n // parts for n in range(parts + 1)]
        if last:
            edges = [tiles - edge for edge in reversed(edges)]
        chunks += [(f, low * LANES, (high - low) * LANES) for low, high in zip(edges, edges[1:])]
    return chunks


def advect_kernel(bands, levs, chunks, lat_t_hbm, lon_t_hbm, shift_hbm, departure_hbm, extents_hbm, area_hbm,
                  fields_ref, moved_ref, lat_t_ref, lon_t_ref, shift_ref, departure_ref, extents_ref,
                  area_ref, held, far_departure, far_extents, far_lat, start_of, weight_of, lon_of, mine, pair, met, plane,
                  below, above, upward, downward, ratio, scalar_sem, load_sem, note_send, note_recv, give_send,
                  give_recv, pass_send, pass_recv, slice_sem, bring_send, bring_recv, keep_sem, table_send,
                  table_recv, chain_send, chain_recv, ready_sem,
                  tail_at, tail_weight, tail_raw, tail_own, tail_up, tail_down, tail_below, tail_above, tail_give_send,
                  tail_give_recv, tail_slice_sem, tail_send, tail_recv, *buffers):
    band, lev = lax.axis_index("lat"), lax.axis_index("lev")
    group, position = band // GROUP, lax.rem(band, GROUP)
    groups = bands // GROUP
    has_up = group < groups - 1
    has_down = group > 0
    rows, field_count, levels, lon_count = fields_ref.shape
    tiles = lon_count // LANES
    tail = tail_of(lon_count)
    last_field = field_count - 1
    count = len(chunks)
    source, mixed = buffers[:count], buffers[count:2 * count]
    column = buffers[2 * count:]
    first_row, total_rows = band * rows, bands * rows
    step_one = 1 - 2 * lax.rem(position, 2)
    step_two = 2 - 4 * (position // 2)
    steps = [step_one, step_two, step_one + step_two]
    partner = {"lev": 1 - lev}
    mates = [{"lat": band + step} for step in steps]
    up_peer, down_peer = {"lat": band + GROUP}, {"lat": band - GROUP}

    def signal(peer):
        pl.semaphore_signal(barrier, inc=1, device_id=peer, device_id_type=MESH)

    barrier = pltpu.get_barrier_semaphore()
    for peer in [partner] + mates[:2]:
        signal(peer)
    pl.when(has_up)(lambda: signal(up_peer))
    pl.when(has_down)(lambda: signal(down_peer))

    scalars = [
        pltpu.make_async_copy(there, here, scalar_sem.at[n])
        for n, (there, here) in enumerate((
            (departure_hbm, departure_ref), (extents_hbm, extents_ref), (lat_t_hbm, lat_t_ref),
            (lon_t_hbm, lon_t_ref), (shift_hbm, shift_ref), (area_hbm, area_ref),
        ))
    ]
    for copy in scalars:
        copy.start()
    load = pltpu.make_async_copy(fields_ref, held, load_sem)
    load.start()

    pl.semaphore_wait(barrier, 3 + has_up.astype(jnp.int32) + has_down.astype(jnp.int32))

    def remote(source_ref, target_ref, send_sem, recv_sem, peer):
        return pltpu.make_async_remote_copy(
            src_ref=source_ref, dst_ref=target_ref, send_sem=send_sem, recv_sem=recv_sem,
            device_id=peer, device_id_type=MESH,
        )

    def width_of(f):
        return (lon_count - (tail * LANES if f == last_field else 0)) // GROUP

    def slice_at(home, k):
        f, first, size = chunks[k]
        width = width_of(f)
        return pl.ds(pl.multiple_of(home * width + first, LANES), size)

    def fields_cut(home, k):
        return fields_ref.at[:, chunks[k][0], :, slice_at(home, k)]

    def source_cut(k, n, blocks=1):
        return source[k].at[pl.ds(n * rows, blocks * rows)]

    def column_cut(home, k):
        f, first, size = chunks[k]
        return column[f].at[:, pl.ds((home * width_of(f) + first) // LANES, size // LANES)]

    def note(n, j):
        here, there = ((departure_ref, far_departure), (extents_ref.at[0], far_extents), (lat_t_ref, far_lat))[n]
        slot, peer = ([(position, mate) for mate in mates] + [(GROUP, up_peer), (GROUP + 1, down_peer)])[j]
        return remote(here, there.at[slot], note_send.at[n, j], note_recv.at[n, j], peer)

    def notes(j, act):
        for n in range(3):
            when_z(j - 3, getattr(note(n, j), act))

    def when_z(j, body):
        if j < 0:
            body()
        else:
            pl.when((has_up, has_down)[j])(body)

    def tail_cut():
        return fields_ref.at[:, last_field, :, pl.ds((tiles - tail) * LANES, tail * LANES)]

    def tail_block(member, first=0, size=None):
        size = tail if size is None else size
        return tail_raw.at[pl.ds(member * rows, rows), :, pl.ds(first * LANES, size * LANES)]

    def tail_give(j):
        if j < 2:
            here, there = tail_cut(), tail_block(position)
        else:
            first = (0, tail // 2, tail)[j - 2:j]
            here = there = tail_block(position + steps[j - 2], first[0], first[1] - first[0])
        return remote(here, there, tail_give_send.at[j], tail_give_recv.at[j], mates[(0, 1, 1, 0)[j]])

    tail_slice = pltpu.make_async_copy(tail_cut(), tail_block(position), tail_slice_sem)
    tail_up_copy = remote(tail_up, tail_below, tail_send.at[0], tail_recv.at[0], up_peer)
    tail_down_copy = remote(tail_down, tail_above, tail_send.at[1], tail_recv.at[1], down_peer)

    def give(j, k):
        home = position + steps[j]
        return remote(
            fields_cut(home, k), source_cut(k, GROUP + position), give_send.at[j], give_recv.at[j, k],
            {"lat": band + steps[j]},
        )

    def own_slice(k):
        return pltpu.make_async_copy(fields_cut(position, k), source_cut(k, GROUP + position), slice_sem.at[k])

    def pass_up(k, block, n, blocks=1):
        return remote(block, source_cut(k, n, blocks), pass_send.at[0], pass_recv.at[0, k], up_peer)

    def pass_down(k, block, n, blocks=1):
        return remote(block, source_cut(k, 2 * GROUP + n, blocks), pass_send.at[1], pass_recv.at[1, k], down_peer)

    def pass_on(k, member, block):
        pl.when(has_up)(pass_up(k, block, member).start)
        pl.when(has_down)(pass_down(k, block, member).start)

    def bring(j, k):
        return remote(
            mixed[k].at[pl.ds((position + steps[j]) * rows, rows)], column_cut(position, k),
            bring_send.at[j], bring_recv.at[j, k], {"lat": band + steps[j]},
        )

    def keep(k):
        return pltpu.make_async_copy(
            mixed[k].at[pl.ds(position * rows, rows)], column_cut(position, k), keep_sem.at[k]
        )

    def table_copy(n):
        if n == 0:
            return remote(mine, met.at[0], table_send.at[0], table_recv.at[0], partner)
        return remote(pair, met.at[n], table_send.at[n], table_recv.at[n], mates[n - 1])

    up_copy = remote(upward, below, chain_send.at[0], chain_recv.at[0], up_peer)
    down_copy = remote(downward, above, chain_send.at[1], chain_recv.at[1], down_peer)

    def give_all(k):
        if k < count:
            for j in range(3):
                give(j, k).start()

    def pass_own(k):
        if k < count:
            pass_on(k, position, fields_cut(position, k))

    def take(k):
        if k >= count:
            if k == count:
                tail_combine()
            return
        for j in range(3):
            give(j, k).wait_recv()
            member = position + steps[j]
            pass_on(k, member, source_cut(k, GROUP + member))

    def tail_prepare(n, slot, member_row):
        north, south = far_extents[slot, 0], far_extents[slot, 1]

        def prepare(row, carry):
            departure = departure_of(far_departure[slot, row], north, south, member_row, rows, total_rows)
            for a, weight in enumerate(cubic(far_lat[slot, row])):
                place = departure - 1 + a - group * GROUP * rows
                inside = jnp.logical_and(place >= 0, place < GROUP * rows)
                tail_at[4 * (n * rows + row) + a] = jnp.where(inside, place, 0)
                tail_weight[4 * (n * rows + row) + a] = jnp.where(inside, weight, 0.0)
            return carry

        lax.fori_loop(0, rows, prepare, 0)

    def tail_mix(n, target):
        def one_row(row, carry):
            places = [tail_at[4 * (n * rows + row) + a] for a in range(4)]
            weights = [tail_weight[4 * (n * rows + row) + a] for a in range(4)]
            for t in range(tail):
                at = pl.ds(t * LANES, LANES)
                total = weights[0] * tail_raw[places[0], :, at]
                for a in range(1, 4):
                    total = total + weights[a] * tail_raw[places[a], :, at]
                target[row, t] = total
            return carry

        lax.fori_loop(0, rows, one_row, 0, unroll=2)

    def tail_combine():
        for j in range(2, 4):
            tail_give(j).wait_recv()
        tail_slice.wait()

        @pl.when(has_up)
        def _():
            tail_mix(2, tail_up)
            tail_up_copy.start()

        @pl.when(has_down)
        def _():
            tail_mix(1, tail_down)
            tail_down_copy.start()

        tail_mix(0, tail_own)

        @pl.when(jnp.logical_not(has_down))
        def _():
            tail_below[...] = jnp.zeros_like(tail_below)

        @pl.when(jnp.logical_not(has_up))
        def _():
            tail_above[...] = jnp.zeros_like(tail_above)

    def tail_add():
        pl.when(has_down)(tail_up_copy.wait_recv)
        pl.when(has_up)(tail_down_copy.wait_recv)

        def one_row(row, carry):
            for t in range(tail):
                column[last_field][row, tiles - tail + t] = tail_own[row, t] + tail_below[row, t] + tail_above[row, t]
            return carry

        lax.fori_loop(0, rows, one_row, 0, unroll=2)

    def combine(k):
        own_slice(k).wait()
        pl.when(has_down)(pass_up(k, source_cut(k, 0, GROUP), 0, GROUP).wait_recv)
        pl.when(has_up)(pass_down(k, source_cut(k, 0, GROUP), 0, GROUP).wait_recv)

        def one_row(n, carry):
            first = start_of[n]
            weights = [weight_of[4 * n + a] for a in range(4)]
            for t in range(chunks[k][2] // LANES):
                at = pl.ds(t * LANES, LANES)
                total = weights[0] * source[k][first, :, at]
                for a in range(1, 4):
                    total = total + weights[a] * source[k][first + a, :, at]
                mixed[k][n, t] = total
            return carry

        lax.fori_loop(0, GROUP * rows, one_row, 0, unroll=4)
        for j in range(3):
            bring(j, k).start()
        keep(k).start()

    def chain(hop):
        if hop == 0:
            total = pair[...]
            for n in range(1, 4):
                table_copy(n).wait_recv()
                total = total + met[n]
            plane[...] = total

            @pl.when(jnp.logical_not(has_down))
            def _():
                below[...] = jnp.zeros_like(below)

            @pl.when(jnp.logical_not(has_up))
            def _():
                above[...] = jnp.zeros_like(above)

        @pl.when(group == hop)
        def _():
            if hop > 0:
                up_copy.wait_recv()
            if hop < groups - 1:
                upward[...] = plane[...] + below[...]
                up_copy.start()

        @pl.when(group == groups - 1 - hop)
        def _():
            if hop > 0:
                down_copy.wait_recv()
            if hop < groups - 1:
                downward[...] = plane[...] + above[...]
                down_copy.start()

    def find_ratio():
        total = plane[...] + below[...] + above[...]
        for f in range(field_count):
            sums_at = total[f:f + 1, :]
            mass_before = jnp.sum(sums_at * total[field_count + 1:field_count + 2, :], axis=1, keepdims=True)
            mass_after = jnp.sum(sums_at * total[field_count:field_count + 1, :], axis=1, keepdims=True)
            ratio[f:f + 1, :] = jnp.broadcast_to(mass_before / mass_after, (1, LANES))

    def along_lon(f):
        for k in range(count):
            if chunks[k][0] == f:
                for j in range(3):
                    block = column_cut(position + steps[j], k)
                    remote(block, block, bring_send.at[j], bring_recv.at[j, k], {"lat": band}).wait_recv()
                keep(k).wait()
        if f == last_field:
            tail_add()
        lane = lax.broadcasted_iota(jnp.int32, (levels, LANES), 1)
        scale = jnp.broadcast_to(ratio[f:f + 1, :], (levels, LANES))

        def one_row(row, carry):
            for t in range(tiles):
                column[f][row, tiles + t] = column[f][row, t]
            column[f][row, 2 * tiles] = column[f][row, 0]
            lon = [lon_of[4 * row + n] * scale for n in range(4)]
            first = lax.rem(shift_ref[row] - 1 + lon_count, lon_count)
            rests = [lax.rem(first + n, LANES) for n in range(4)]
            turns = [lax.rem(LANES - rest, LANES) for rest in rests]
            stays = [lane < LANES - rest for rest in rests]
            bases = [(first + n) // LANES for n in range(4)]

            def turned(t):
                return [pltpu.roll(column[f][row, bases[n] + t], turns[n], 1) for n in range(4)]

            here = turned(0)
            for t in range(tiles):
                there = turned(t + 1)
                total = lon[0] * jnp.where(stays[0], here[0], there[0])
                for n in range(1, 4):
                    total = total + lon[n] * jnp.where(stays[n], here[n], there[n])
                moved_ref[row, f, :, pl.ds(t * LANES, LANES)] = total
                here = there
            return carry

        lax.fori_loop(0, rows, one_row, 0, unroll=ROLL)

    pl.semaphore_signal(ready_sem, inc=1, device_id=mates[0], device_id_type=MESH)
    pass_own(0)
    for j in range(2):
        give(j, 0).start()
    for k in range(1, OWN):
        pass_own(k)
    pl.semaphore_wait(ready_sem, 1)
    give(2, 0).start()
    for copy in scalars:
        copy.wait()
    for j in range(5):
        notes(j, "start")
    give_all(1)
    load.wait()
    lane = lax.broadcasted_iota(jnp.int32, (1, mine.shape[1]), 1)
    taken = jnp.zeros(lane.shape, jnp.float32)
    for row in range(rows):
        departure = departure_of(
            departure_ref[row], extents_ref[0, 0], extents_ref[0, 1], first_row, rows, total_rows
        )
        lon_w = cubic(lon_t_ref[row])
        for n, weight in enumerate(lon_w):
            lon_of[4 * row + n] = weight
        share = area_ref[first_row + row] * (lon_w[0] + lon_w[1] + lon_w[2] + lon_w[3]) * (1.0 / levs)
        for a, weight in enumerate(cubic(lat_t_ref[row])):
            taken = taken + jnp.where(lane == departure - 1 + a, share * weight, 0.0)
    sums = [jnp.zeros(lane.shape, jnp.float32) for _ in range(field_count)]
    before = jnp.zeros(lane.shape, jnp.float32)
    for row in range(rows):
        before = before + jnp.where(lane == first_row + row, area_ref[first_row + row] * (1.0 / levs), 0.0)
        for f in range(field_count):
            total = jnp.sum(jnp.sum(held[row, f], axis=0, keepdims=True), axis=1, keepdims=True)
            sums[f] = sums[f] + jnp.where(lane == first_row + row, total, 0.0)
    mine[...] = jnp.zeros_like(mine)
    for f in range(field_count):
        mine[f:f + 1, :] = sums[f]
    mine[field_count:field_count + 1, :] = taken
    mine[field_count + 1:field_count + 2, :] = before
    table_copy(0).start()
    for k in range(count):
        own_slice(k).start()
    tail_slice.start()
    table_copy(0).wait_recv()
    pair[...] = mine[...] + met[0]
    for n in range(1, 4):
        table_copy(n).start()
    for k in range(2, GIVEN):
        give_all(k)
    for k in range(PASSED):
        take(k)
    for row in range(rows):
        far_departure[position, row] = departure_ref[row]
        far_lat[position, row] = lat_t_ref[row]
    for e in range(2):
        far_extents[position, e] = extents_ref[0, e]
    for n in range(3):
        for j in range(3):
            note(n, j).wait_recv()
        pl.when(has_down)(note(n, 3).wait_recv)
        pl.when(has_up)(note(n, 4).wait_recv)
    for member in range(GROUP):
        member_row = (group * GROUP + member) * rows
        north, south = far_extents[member, 0], far_extents[member, 1]

        def prepare(row, carry):
            departure = departure_of(far_departure[member, row], north, south, member_row, rows, total_rows)
            start_of[member * rows + row] = departure - 1 - (group - 1) * GROUP * rows
            for a, weight in enumerate(cubic(far_lat[member, row])):
                weight_of[4 * (member * rows + row) + a] = weight
            return carry

        lax.fori_loop(0, rows, prepare, 0)
    chain(0)
    tail_prepare(0, position, first_row)
    pl.when(has_down)(lambda: tail_prepare(1, GROUP, first_row - GROUP * rows))
    pl.when(has_up)(lambda: tail_prepare(2, GROUP + 1, first_row + GROUP * rows))

    hop = 1
    finished = 0
    for k in range(count):
        give_all(k + GIVEN)
        pass_own(k + OWN)
        take(k + PASSED)
        if k == TAIL_GIVE:
            for j in range(2):
                tail_give(j).start()
        if k == TAIL_RELAY:
            for j in range(2):
                tail_give(j).wait_recv()
                tail_give(j + 2).start()
        combine(k)
        while hop < groups and (hop * (count - WAIT)) // groups <= k:
            chain(hop)
            hop += 1
            if hop == groups:
                find_ratio()
        if k < count - 1 and hop == groups and chunks[k - WAIT][0] > finished:
            along_lon(finished)
            finished += 1
    for f in range(finished, field_count):
        along_lon(f)

    for k in range(count):
        for j in range(3):
            give(j, k).wait_send()
            bring(j, k).wait_send()
        pl.when(has_up)(pass_up(k, source_cut(k, 0, GROUP), 0, GROUP).wait_send)
        pl.when(has_down)(pass_down(k, source_cut(k, 0, GROUP), 0, GROUP).wait_send)
    for j in range(5):
        notes(j, "wait_send")
    for n in range(4):
        table_copy(n).wait_send()
    for j in range(4):
        tail_give(j).wait_send()
    pl.when(has_up)(tail_up_copy.wait_send)
    pl.when(has_down)(tail_down_copy.wait_send)
    pl.when(has_up)(up_copy.wait_send)
    pl.when(has_down)(down_copy.wait_send)


def advect(lat_t, lon_t, shift, departure_row, extents, area, fields):
    bands, levs = lax.axis_size("lat"), lax.axis_size("lev")
    rows, field_count, levels, lon_count = fields.shape
    table = (-(-(field_count + 2) // 8) * 8, -(-bands * rows // LANES) * LANES)
    tail = tail_of(lon_count)
    tail_block = pltpu.VMEM((rows, tail, levels, LANES), jnp.float32)
    chunks = chunks_of(field_count, lon_count)
    count = len(chunks)
    dma = pltpu.SemaphoreType.DMA
    hbm = pl.BlockSpec(memory_space=pltpu.HBM)
    operands = (lat_t, lon_t, shift, departure_row, extents, area, fields)
    return pl.pallas_call(
        functools.partial(advect_kernel, bands, levs, chunks),
        out_shape=jax.ShapeDtypeStruct(fields.shape, fields.dtype),
        in_specs=[hbm] * 7,
        out_specs=pl.BlockSpec(memory_space=pltpu.VMEM),
        scratch_shapes=[
            pltpu.SMEM(lat_t.shape, jnp.float32),
            pltpu.SMEM(lon_t.shape, jnp.float32),
            pltpu.SMEM(shift.shape, jnp.int32),
            pltpu.SMEM(departure_row.shape, jnp.int32),
            pltpu.SMEM(extents.shape, jnp.int32),
            pltpu.SMEM(area.shape, jnp.float32),
            pltpu.VMEM(fields.shape, jnp.float32),
            pltpu.SMEM((GROUP + 2, rows), jnp.int32),
            pltpu.SMEM((GROUP + 2, 2), jnp.int32),
            pltpu.SMEM((GROUP + 2, rows), jnp.float32),
            pltpu.SMEM((GROUP * rows,), jnp.int32),
            pltpu.SMEM((4 * GROUP * rows,), jnp.float32),
            pltpu.SMEM((4 * rows,), jnp.float32),
            pltpu.VMEM(table, jnp.float32),
            pltpu.VMEM(table, jnp.float32),
            pltpu.VMEM((4,) + table, jnp.float32),
        ]
        + [pltpu.VMEM(table, jnp.float32)] * 5
        + [
            pltpu.VMEM((table[0], LANES), jnp.float32),
            dma((6,)),
            dma,
            dma((3, 5)),
            dma((3, 5)),
            dma((3,)),
            dma((3, count)),
            dma((2,)),
            dma((2, count)),
            dma((count,)),
            dma((3,)),
            dma((3, count)),
            dma((count,)),
            dma((4,)),
            dma((4,)),
            dma((2,)),
            dma((2,)),
            pltpu.SemaphoreType.REGULAR,
            pltpu.SMEM((12 * rows,), jnp.int32),
            pltpu.SMEM((12 * rows,), jnp.float32),
            pltpu.VMEM((GROUP * rows, levels, tail * LANES), jnp.float32),
        ]
        + [tail_block] * 5
        + [
            dma((4,)),
            dma((4,)),
            dma,
            dma((2,)),
            dma((2,)),
        ]
        + [pltpu.VMEM((3 * GROUP * rows, levels, size), jnp.float32) for _, _, size in chunks]
        + [pltpu.VMEM((GROUP * rows, size // LANES, levels, LANES), jnp.float32) for _, _, size in chunks]
        + [pltpu.VMEM((rows, 2 * lon_count // LANES + 1, levels, LANES), jnp.float32)] * field_count,
        compiler_params=pltpu.CompilerParams(
            collective_id=0, has_side_effects=True, vmem_limit_bytes=VMEM_BYTES
        ),
        name="advect",
    )(*[pltpu.with_memory_space_constraint(x, pltpu.HBM) for x in operands])


def per_device(fields, lat_fraction, lon_fraction, lon_shift, departure_row, extents):
    bands = lax.axis_size("lat")
    total_rows = bands * fields.shape[0]
    row_ids = np.arange(-(-total_rows // LANES) * LANES)
    area = np.where(row_ids < total_rows, np.cos(math.pi * (row_ids + 0.5) / total_rows - math.pi / 2.0), 0.0)
    area = jnp.asarray(area, jnp.float32)
    return advect(lat_fraction, lon_fraction, lon_shift, departure_row, extents, area, fields)


def solution(mesh):
    return jax.shard_map(
        per_device,
        mesh=mesh,
        in_specs=(
            P("lat", None, "lev", None),
            P("lat"),
            P("lat"),
            P("lat"),
            P("lat"),
            P("lat", None),
        ),
        out_specs=P("lat", None, "lev", None),
        check_vma=False,
    )
```

```python
import functools
import math

import jax
import jax.numpy as jnp
import numpy as np
from jax import lax
from jax.experimental import pallas as pl
from jax.experimental.pallas import tpu as pltpu
from jax.sharding import PartitionSpec as P

GROUP = 4
LANES = 128
PARTS = (2, 3, 3)
TAIL = 4
GIVEN = 6
PASSED = 3
WAIT = 1
ROLL = 5
OWN = 3
TAIL_GIVE = 0
TAIL_RELAY = 2
VMEM_BYTES = 40 * 1024 * 1024
MESH = pl.DeviceIdType.MESH


def cubic(t):
    sixth = 1.0 / 6.0
    return (
        -t * (t - 1.0) * (t - 2.0) * sixth,
        (t + 1.0) * (t - 1.0) * (t - 2.0) * 0.5,
        -(t + 1.0) * t * (t - 2.0) * 0.5,
        (t + 1.0) * t * (t - 1.0) * sixth,
    )


def departure_of(departure, north, south, first_row, rows, total_rows):
    low = first_row - north * rows + 1
    high = first_row + rows - 3 + south * rows
    inside = jnp.minimum(jnp.maximum(departure, low), high)
    return jnp.minimum(jnp.maximum(inside, 1), total_rows - 3)


def tail_of(lon_count):
    tiles = lon_count // LANES
    return TAIL + (tiles - TAIL) % GROUP


def chunks_of(field_count, lon_count):
    chunks = []
    for f in range(field_count):
        last = f == field_count - 1
        tiles = (lon_count // LANES - (tail_of(lon_count) if last else 0)) // GROUP
        parts = min(PARTS[min(f, len(PARTS) - 1)], tiles)
        edges = [tiles * n // parts for n in range(parts + 1)]
        if last:
            edges = [tiles - edge for edge in reversed(edges)]
        chunks += [(f, low * LANES, (high - low) * LANES) for low, high in zip(edges, edges[1:])]
    return chunks


def advect_kernel(bands, levs, chunks, lat_t_hbm, lon_t_hbm, shift_hbm, departure_hbm, extents_hbm, area_hbm,
                  fields_ref, moved_ref, lat_t_ref, lon_t_ref, shift_ref, departure_ref, extents_ref,
                  area_ref, held, far_departure, far_extents, far_lat, start_of, weight_of, lon_of, mine, pair, met, plane,
                  below, above, upward, downward, ratio, scalar_sem, load_sem, note_send, note_recv, give_send,
                  give_recv, pass_send, pass_recv, slice_sem, bring_send, bring_recv, keep_sem, table_send,
                  table_recv, chain_send, chain_recv, ready_sem,
                  tail_at, tail_weight, tail_raw, tail_own, tail_up, tail_down, tail_below, tail_above, tail_give_send,
                  tail_give_recv, tail_slice_sem, tail_send, tail_recv, *buffers):
    band, lev = lax.axis_index("lat"), lax.axis_index("lev")
    group, position = band // GROUP, lax.rem(band, GROUP)
    groups = bands // GROUP
    has_up = group < groups - 1
    has_down = group > 0
    rows, field_count, levels, lon_count = fields_ref.shape
    tiles = lon_count // LANES
    tail = tail_of(lon_count)
    last_field = field_count - 1
    count = len(chunks)
    source, mixed = buffers[:count], buffers[count:2 * count]
    column = buffers[2 * count:]
    first_row, total_rows = band * rows, bands * rows
    step_one = 1 - 2 * lax.rem(position, 2)
    step_two = 2 - 4 * (position // 2)
    steps = [step_one, step_two, step_one + step_two]
    partner = {"lev": 1 - lev}
    mates = [{"lat": band + step} for step in steps]
    up_peer, down_peer = {"lat": band + GROUP}, {"lat": band - GROUP}

    def signal(peer):
        pl.semaphore_signal(barrier, inc=1, device_id=peer, device_id_type=MESH)

    barrier = pltpu.get_barrier_semaphore()
    for peer in [partner] + mates[:2]:
        signal(peer)
    pl.when(has_up)(lambda: signal(up_peer))
    pl.when(has_down)(lambda: signal(down_peer))

    scalars = [
        pltpu.make_async_copy(there, here, scalar_sem.at[n])
        for n, (there, here) in enumerate((
            (departure_hbm, departure_ref), (extents_hbm, extents_ref), (lat_t_hbm, lat_t_ref),
            (lon_t_hbm, lon_t_ref), (shift_hbm, shift_ref), (area_hbm, area_ref),
        ))
    ]
    for copy in scalars:
        copy.start()
    load = pltpu.make_async_copy(fields_ref, held, load_sem)
    load.start()

    pl.semaphore_wait(barrier, 3 + has_up.astype(jnp.int32) + has_down.astype(jnp.int32))

    def remote(source_ref, target_ref, send_sem, recv_sem, peer):
        return pltpu.make_async_remote_copy(
            src_ref=source_ref, dst_ref=target_ref, send_sem=send_sem, recv_sem=recv_sem,
            device_id=peer, device_id_type=MESH,
        )

    def width_of(f):
        return (lon_count - (tail * LANES if f == last_field else 0)) // GROUP

    def slice_at(home, k):
        f, first, size = chunks[k]
        width = width_of(f)
        return pl.ds(pl.multiple_of(home * width + first, LANES), size)

    def fields_cut(home, k):
        return fields_ref.at[:, chunks[k][0], :, slice_at(home, k)]

    def source_cut(k, n, blocks=1):
        return source[k].at[pl.ds(n * rows, blocks * rows)]

    def column_cut(home, k):
        f, first, size = chunks[k]
        return column[f].at[:, pl.ds((home * width_of(f) + first) // LANES, size // LANES)]

    def note(n, j):
        here, there = ((departure_ref, far_departure), (extents_ref.at[0], far_extents), (lat_t_ref, far_lat))[n]
        slot, peer = ([(position, mate) for mate in mates] + [(GROUP, up_peer), (GROUP + 1, down_peer)])[j]
        return remote(here, there.at[slot], note_send.at[n, j], note_recv.at[n, j], peer)

    def notes(j, act):
        for n in range(3):
            when_z(j - 3, getattr(note(n, j), act))

    def when_z(j, body):
        if j < 0:
            body()
        else:
            pl.when((has_up, has_down)[j])(body)

    def tail_cut():
        return fields_ref.at[:, last_field, :, pl.ds((tiles - tail) * LANES, tail * LANES)]

    def tail_block(member, first=0, size=None):
        size = tail if size is None else size
        return tail_raw.at[pl.ds(member * rows, rows), :, pl.ds(first * LANES, size * LANES)]

    def tail_give(j):
        if j < 2:
            here, there = tail_cut(), tail_block(position)
        else:
            first = (0, tail // 2, tail)[j - 2:j]
            here = there = tail_block(position + steps[j - 2], first[0], first[1] - first[0])
        return remote(here, there, tail_give_send.at[j], tail_give_recv.at[j], mates[(0, 1, 1, 0)[j]])

    tail_slice = pltpu.make_async_copy(tail_cut(), tail_block(position), tail_slice_sem)
    tail_up_copy = remote(tail_up, tail_below, tail_send.at[0], tail_recv.at[0], up_peer)
    tail_down_copy = remote(tail_down, tail_above, tail_send.at[1], tail_recv.at[1], down_peer)

    def give(j, k):
        home = position + steps[j]
        return remote(
            fields_cut(home, k), source_cut(k, GROUP + position), give_send.at[j], give_recv.at[j, k],
            {"lat": band + steps[j]},
        )

    def own_slice(k):
        return pltpu.make_async_copy(fields_cut(position, k), source_cut(k, GROUP + position), slice_sem.at[k])

    def pass_up(k, block, n, blocks=1):
        return remote(block, source_cut(k, n, blocks), pass_send.at[0], pass_recv.at[0, k], up_peer)

    def pass_down(k, block, n, blocks=1):
        return remote(block, source_cut(k, 2 * GROUP + n, blocks), pass_send.at[1], pass_recv.at[1, k], down_peer)

    def pass_on(k, member, block):
        pl.when(has_up)(pass_up(k, block, member).start)
        pl.when(has_down)(pass_down(k, block, member).start)

    def bring(j, k):
        return remote(
            mixed[k].at[pl.ds((position + steps[j]) * rows, rows)], column_cut(position, k),
            bring_send.at[j], bring_recv.at[j, k], {"lat": band + steps[j]},
        )

    def keep(k):
        return pltpu.make_async_copy(
            mixed[k].at[pl.ds(position * rows, rows)], column_cut(position, k), keep_sem.at[k]
        )

    def table_copy(n):
        if n == 0:
            return remote(mine, met.at[0], table_send.at[0], table_recv.at[0], partner)
        return remote(pair, met.at[n], table_send.at[n], table_recv.at[n], mates[n - 1])

    up_copy = remote(upward, below, chain_send.at[0], chain_recv.at[0], up_peer)
    down_copy = remote(downward, above, chain_send.at[1], chain_recv.at[1], down_peer)

    def give_all(k):
        if k < count:
            for j in range(3):
                give(j, k).start()

    def pass_own(k):
        if k < count:
            pass_on(k, position, fields_cut(position, k))

    def take(k):
        if k >= count:
            if k == count:
                tail_combine()
            return
        for j in range(3):
            give(j, k).wait_recv()
            member = position + steps[j]
            pass_on(k, member, source_cut(k, GROUP + member))

    def tail_prepare(n, slot, member_row):
        north, south = far_extents[slot, 0], far_extents[slot, 1]

        def prepare(row, carry):
            departure = departure_of(far_departure[slot, row], north, south, member_row, rows, total_rows)
            for a, weight in enumerate(cubic(far_lat[slot, row])):
                place = departure - 1 + a - group * GROUP * rows
                inside = jnp.logical_and(place >= 0, place < GROUP * rows)
                tail_at[4 * (n * rows + row) + a] = jnp.where(inside, place, 0)
                tail_weight[4 * (n * rows + row) + a] = jnp.where(inside, weight, 0.0)
            return carry

        lax.fori_loop(0, rows, prepare, 0)

    def tail_mix(n, target):
        def one_row(row, carry):
            places = [tail_at[4 * (n * rows + row) + a] for a in range(4)]
            weights = [tail_weight[4 * (n * rows + row) + a] for a in range(4)]
            for t in range(tail):
                at = pl.ds(t * LANES, LANES)
                total = weights[0] * tail_raw[places[0], :, at]
                for a in range(1, 4):
                    total = total + weights[a] * tail_raw[places[a], :, at]
                target[row, t] = total
            return carry

        lax.fori_loop(0, rows, one_row, 0, unroll=2)

    def tail_combine():
        for j in range(2, 4):
            tail_give(j).wait_recv()
        tail_slice.wait()

        @pl.when(has_up)
        def _():
            tail_mix(2, tail_up)
            tail_up_copy.start()

        @pl.when(has_down)
        def _():
            tail_mix(1, tail_down)
            tail_down_copy.start()

        tail_mix(0, tail_own)

        @pl.when(jnp.logical_not(has_down))
        def _():
            tail_below[...] = jnp.zeros_like(tail_below)

        @pl.when(jnp.logical_not(has_up))
        def _():
            tail_above[...] = jnp.zeros_like(tail_above)

    def tail_add():
        pl.when(has_down)(tail_up_copy.wait_recv)
        pl.when(has_up)(tail_down_copy.wait_recv)

        def one_row(row, carry):
            for t in range(tail):
                total = tail_own[row, t] + tail_below[row, t] + tail_above[row, t]
                column[last_field][row, tiles - tail + t] = total
                column[last_field][row, 2 * tiles - tail + t] = total
            return carry

        lax.fori_loop(0, rows, one_row, 0, unroll=2)

    def combine(k):
        own_slice(k).wait()
        pl.when(has_down)(pass_up(k, source_cut(k, 0, GROUP), 0, GROUP).wait_recv)
        pl.when(has_up)(pass_down(k, source_cut(k, 0, GROUP), 0, GROUP).wait_recv)

        def one_row(n, carry):
            first = start_of[n]
            weights = [weight_of[4 * n + a] for a in range(4)]
            for t in range(chunks[k][2] // LANES):
                at = pl.ds(t * LANES, LANES)
                total = weights[0] * source[k][first, :, at]
                for a in range(1, 4):
                    total = total + weights[a] * source[k][first + a, :, at]
                mixed[k][n, t] = total
            return carry

        lax.fori_loop(0, GROUP * rows, one_row, 0, unroll=4)
        for j in range(3):
            bring(j, k).start()
        keep(k).start()

    def chain(hop):
        if hop == 0:
            total = pair[...]
            for n in range(1, 4):
                table_copy(n).wait_recv()
                total = total + met[n]
            plane[...] = total

            @pl.when(jnp.logical_not(has_down))
            def _():
                below[...] = jnp.zeros_like(below)

            @pl.when(jnp.logical_not(has_up))
            def _():
                above[...] = jnp.zeros_like(above)

        @pl.when(group == hop)
        def _():
            if hop > 0:
                up_copy.wait_recv()
            if hop < groups - 1:
                upward[...] = plane[...] + below[...]
                up_copy.start()

        @pl.when(group == groups - 1 - hop)
        def _():
            if hop > 0:
                down_copy.wait_recv()
            if hop < groups - 1:
                downward[...] = plane[...] + above[...]
                down_copy.start()

    def find_ratio():
        total = plane[...] + below[...] + above[...]
        for f in range(field_count):
            sums_at = total[f:f + 1, :]
            mass_before = jnp.sum(sums_at * total[field_count + 1:field_count + 2, :], axis=1, keepdims=True)
            mass_after = jnp.sum(sums_at * total[field_count:field_count + 1, :], axis=1, keepdims=True)
            ratio[f:f + 1, :] = jnp.broadcast_to(mass_before / mass_after, (1, LANES))

    def repeat(f, places):
        def one_row(row, carry):
            for t in places:
                column[f][row, tiles + t] = column[f][row, t]
                if t == 0:
                    column[f][row, 2 * tiles] = column[f][row, t]
            return carry

        lax.fori_loop(0, rows, one_row, 0, unroll=2)

    def along_lon(f):
        for k in range(count):
            if chunks[k][0] == f:
                for j in range(3):
                    block = column_cut(position + steps[j], k)
                    remote(block, block, bring_send.at[j], bring_recv.at[j, k], {"lat": band}).wait_recv()
                keep(k).wait()
                first, size = chunks[k][1:]
                starts = [(home * width_of(f) + first) // LANES for home in range(GROUP)]
                repeat(f, [start + t for start in starts for t in range(size // LANES)])
        if f == last_field:
            tail_add()
        lane = lax.broadcasted_iota(jnp.int32, (levels, LANES), 1)
        scale = jnp.broadcast_to(ratio[f:f + 1, :], (levels, LANES))

        def one_row(row, carry):
            lon = [lon_of[4 * row + n] * scale for n in range(4)]
            first = lax.rem(shift_ref[row] - 1 + lon_count, lon_count)
            rests = [lax.rem(first + n, LANES) for n in range(4)]
            turns = [lax.rem(LANES - rest, LANES) for rest in rests]
            stays = [lane < LANES - rest for rest in rests]
            bases = [(first + n) // LANES for n in range(4)]

            def turned(t):
                return [pltpu.roll(column[f][row, bases[n] + t], turns[n], 1) for n in range(4)]

            here = turned(0)
            for t in range(tiles):
                there = turned(t + 1)
                total = lon[0] * jnp.where(stays[0], here[0], there[0])
                for n in range(1, 4):
                    total = total + lon[n] * jnp.where(stays[n], here[n], there[n])
                moved_ref[row, f, :, pl.ds(t * LANES, LANES)] = total
                here = there
            return carry

        lax.fori_loop(0, rows, one_row, 0, unroll=ROLL)

    pl.semaphore_signal(ready_sem, inc=1, device_id=mates[0], device_id_type=MESH)
    pass_own(0)
    for j in range(2):
        give(j, 0).start()
    for k in range(1, OWN):
        pass_own(k)
    pl.semaphore_wait(ready_sem, 1)
    give(2, 0).start()
    for copy in scalars:
        copy.wait()
    for j in range(5):
        notes(j, "start")
    give_all(1)
    load.wait()
    lane = lax.broadcasted_iota(jnp.int32, (1, mine.shape[1]), 1)
    taken = jnp.zeros(lane.shape, jnp.float32)
    for row in range(rows):
        departure = departure_of(
            departure_ref[row], extents_ref[0, 0], extents_ref[0, 1], first_row, rows, total_rows
        )
        lon_w = cubic(lon_t_ref[row])
        for n, weight in enumerate(lon_w):
            lon_of[4 * row + n] = weight
        share = area_ref[first_row + row] * (lon_w[0] + lon_w[1] + lon_w[2] + lon_w[3]) * (1.0 / levs)
        for a, weight in enumerate(cubic(lat_t_ref[row])):
            taken = taken + jnp.where(lane == departure - 1 + a, share * weight, 0.0)
    sums = [jnp.zeros(lane.shape, jnp.float32) for _ in range(field_count)]
    before = jnp.zeros(lane.shape, jnp.float32)
    for row in range(rows):
        before = before + jnp.where(lane == first_row + row, area_ref[first_row + row] * (1.0 / levs), 0.0)
        for f in range(field_count):
            total = jnp.sum(jnp.sum(held[row, f], axis=0, keepdims=True), axis=1, keepdims=True)
            sums[f] = sums[f] + jnp.where(lane == first_row + row, total, 0.0)
    mine[...] = jnp.zeros_like(mine)
    for f in range(field_count):
        mine[f:f + 1, :] = sums[f]
    mine[field_count:field_count + 1, :] = taken
    mine[field_count + 1:field_count + 2, :] = before
    table_copy(0).start()
    for k in range(count):
        own_slice(k).start()
    tail_slice.start()
    table_copy(0).wait_recv()
    pair[...] = mine[...] + met[0]
    for n in range(1, 4):
        table_copy(n).start()
    for k in range(2, GIVEN):
        give_all(k)
    for k in range(PASSED):
        take(k)
    for row in range(rows):
        far_departure[position, row] = departure_ref[row]
        far_lat[position, row] = lat_t_ref[row]
    for e in range(2):
        far_extents[position, e] = extents_ref[0, e]
    for n in range(3):
        for j in range(3):
            note(n, j).wait_recv()
        pl.when(has_down)(note(n, 3).wait_recv)
        pl.when(has_up)(note(n, 4).wait_recv)
    for member in range(GROUP):
        member_row = (group * GROUP + member) * rows
        north, south = far_extents[member, 0], far_extents[member, 1]

        def prepare(row, carry):
            departure = departure_of(far_departure[member, row], north, south, member_row, rows, total_rows)
            start_of[member * rows + row] = departure - 1 - (group - 1) * GROUP * rows
            for a, weight in enumerate(cubic(far_lat[member, row])):
                weight_of[4 * (member * rows + row) + a] = weight
            return carry

        lax.fori_loop(0, rows, prepare, 0)
    chain(0)
    tail_prepare(0, position, first_row)
    pl.when(has_down)(lambda: tail_prepare(1, GROUP, first_row - GROUP * rows))
    pl.when(has_up)(lambda: tail_prepare(2, GROUP + 1, first_row + GROUP * rows))

    hop = 1
    finished = 0
    for k in range(count):
        give_all(k + GIVEN)
        pass_own(k + OWN)
        take(k + PASSED)
        if k == TAIL_GIVE:
            for j in range(2):
                tail_give(j).start()
        if k == TAIL_RELAY:
            for j in range(2):
                tail_give(j).wait_recv()
                tail_give(j + 2).start()
        combine(k)
        while hop < groups and (hop * (count - WAIT)) // groups <= k:
            chain(hop)
            hop += 1
            if hop == groups:
                find_ratio()
        if k < count - 1 and hop == groups and chunks[k - WAIT][0] > finished:
            along_lon(finished)
            finished += 1
    for k in range(count):
        for j in range(3):
            give(j, k).wait_send()
        pl.when(has_up)(pass_up(k, source_cut(k, 0, GROUP), 0, GROUP).wait_send)
        pl.when(has_down)(pass_down(k, source_cut(k, 0, GROUP), 0, GROUP).wait_send)
    for j in range(5):
        notes(j, "wait_send")
    for n in range(4):
        table_copy(n).wait_send()
    for j in range(4):
        tail_give(j).wait_send()
    pl.when(has_up)(up_copy.wait_send)
    pl.when(has_down)(down_copy.wait_send)
    for f in range(finished, field_count):
        along_lon(f)
    for k in range(count):
        for j in range(3):
            bring(j, k).wait_send()
    pl.when(has_up)(tail_up_copy.wait_send)
    pl.when(has_down)(tail_down_copy.wait_send)


def advect(lat_t, lon_t, shift, departure_row, extents, area, fields):
    bands, levs = lax.axis_size("lat"), lax.axis_size("lev")
    rows, field_count, levels, lon_count = fields.shape
    table = (-(-(field_count + 2) // 8) * 8, -(-bands * rows // LANES) * LANES)
    tail = tail_of(lon_count)
    tail_block = pltpu.VMEM((rows, tail, levels, LANES), jnp.float32)
    chunks = chunks_of(field_count, lon_count)
    count = len(chunks)
    dma = pltpu.SemaphoreType.DMA
    hbm = pl.BlockSpec(memory_space=pltpu.HBM)
    operands = (lat_t, lon_t, shift, departure_row, extents, area, fields)
    return pl.pallas_call(
        functools.partial(advect_kernel, bands, levs, chunks),
        out_shape=jax.ShapeDtypeStruct(fields.shape, fields.dtype),
        in_specs=[hbm] * 7,
        out_specs=pl.BlockSpec(memory_space=pltpu.VMEM),
        scratch_shapes=[
            pltpu.SMEM(lat_t.shape, jnp.float32),
            pltpu.SMEM(lon_t.shape, jnp.float32),
            pltpu.SMEM(shift.shape, jnp.int32),
            pltpu.SMEM(departure_row.shape, jnp.int32),
            pltpu.SMEM(extents.shape, jnp.int32),
            pltpu.SMEM(area.shape, jnp.float32),
            pltpu.VMEM(fields.shape, jnp.float32),
            pltpu.SMEM((GROUP + 2, rows), jnp.int32),
            pltpu.SMEM((GROUP + 2, 2), jnp.int32),
            pltpu.SMEM((GROUP + 2, rows), jnp.float32),
            pltpu.SMEM((GROUP * rows,), jnp.int32),
            pltpu.SMEM((4 * GROUP * rows,), jnp.float32),
            pltpu.SMEM((4 * rows,), jnp.float32),
            pltpu.VMEM(table, jnp.float32),
            pltpu.VMEM(table, jnp.float32),
            pltpu.VMEM((4,) + table, jnp.float32),
        ]
        + [pltpu.VMEM(table, jnp.float32)] * 5
        + [
            pltpu.VMEM((table[0], LANES), jnp.float32),
            dma((6,)),
            dma,
            dma((3, 5)),
            dma((3, 5)),
            dma((3,)),
            dma((3, count)),
            dma((2,)),
            dma((2, count)),
            dma((count,)),
            dma((3,)),
            dma((3, count)),
            dma((count,)),
            dma((4,)),
            dma((4,)),
            dma((2,)),
            dma((2,)),
            pltpu.SemaphoreType.REGULAR,
            pltpu.SMEM((12 * rows,), jnp.int32),
            pltpu.SMEM((12 * rows,), jnp.float32),
            pltpu.VMEM((GROUP * rows, levels, tail * LANES), jnp.float32),
        ]
        + [tail_block] * 5
        + [
            dma((4,)),
            dma((4,)),
            dma,
            dma((2,)),
            dma((2,)),
        ]
        + [pltpu.VMEM((3 * GROUP * rows, levels, size), jnp.float32) for _, _, size in chunks]
        + [pltpu.VMEM((GROUP * rows, size // LANES, levels, LANES), jnp.float32) for _, _, size in chunks]
        + [pltpu.VMEM((rows, 2 * lon_count // LANES + 1, levels, LANES), jnp.float32)] * field_count,
        compiler_params=pltpu.CompilerParams(
            collective_id=0, has_side_effects=True, vmem_limit_bytes=VMEM_BYTES
        ),
        name="advect",
    )(*[pltpu.with_memory_space_constraint(x, pltpu.HBM) for x in operands])


def per_device(fields, lat_fraction, lon_fraction, lon_shift, departure_row, extents):
    bands = lax.axis_size("lat")
    total_rows = bands * fields.shape[0]
    row_ids = np.arange(-(-total_rows // LANES) * LANES)
    area = np.where(row_ids < total_rows, np.cos(math.pi * (row_ids + 0.5) / total_rows - math.pi / 2.0), 0.0)
    area = jnp.asarray(area, jnp.float32)
    return advect(lat_fraction, lon_fraction, lon_shift, departure_row, extents, area, fields)


def solution(mesh):
    return jax.shard_map(
        per_device,
        mesh=mesh,
        in_specs=(
            P("lat", None, "lev", None),
            P("lat"),
            P("lat"),
            P("lat"),
            P("lat"),
            P("lat", None),
        ),
        out_specs=P("lat", None, "lev", None),
        check_vma=False,
    )
```

```python
import functools
import math

import jax
import jax.numpy as jnp
import numpy as np
from jax import lax
from jax.experimental import pallas as pl
from jax.experimental.pallas import tpu as pltpu
from jax.sharding import PartitionSpec as P

GROUP = 4
LANES = 128
PARTS = (2, 3, 3)
TAIL = 4
GIVEN = 6
PASSED = 3
WAIT = 1
ROLL = 5
OWN = 3
TAIL_GIVE = 0
TAIL_RELAY = 2
VMEM_BYTES = 40 * 1024 * 1024
MESH = pl.DeviceIdType.MESH


def cubic(t):
    sixth = 1.0 / 6.0
    return (
        -t * (t - 1.0) * (t - 2.0) * sixth,
        (t + 1.0) * (t - 1.0) * (t - 2.0) * 0.5,
        -(t + 1.0) * t * (t - 2.0) * 0.5,
        (t + 1.0) * t * (t - 1.0) * sixth,
    )


def departure_of(departure, north, south, first_row, rows, total_rows):
    low = first_row - north * rows + 1
    high = first_row + rows - 3 + south * rows
    inside = jnp.minimum(jnp.maximum(departure, low), high)
    return jnp.minimum(jnp.maximum(inside, 1), total_rows - 3)


def tail_of(lon_count):
    tiles = lon_count // LANES
    return TAIL + (tiles - TAIL) % GROUP


def chunks_of(field_count, lon_count):
    chunks = []
    for f in range(field_count):
        last = f == field_count - 1
        tiles = (lon_count // LANES - (tail_of(lon_count) if last else 0)) // GROUP
        parts = min(PARTS[min(f, len(PARTS) - 1)], tiles)
        edges = [tiles * n // parts for n in range(parts + 1)]
        if last:
            edges = [tiles - edge for edge in reversed(edges)]
        chunks += [(f, low * LANES, (high - low) * LANES) for low, high in zip(edges, edges[1:])]
    return chunks


def advect_kernel(bands, levs, chunks, lat_t_hbm, lon_t_hbm, shift_hbm, departure_hbm, extents_hbm, area_hbm,
                  fields_ref, moved_ref, lat_t_ref, lon_t_ref, shift_ref, departure_ref, extents_ref,
                  area_ref, held, far_departure, far_extents, far_lat, start_of, weight_of, lon_of, mine, pair, met, plane,
                  below, above, upward, downward, ratio, scalar_sem, load_sem, note_send, note_recv, give_send,
                  give_recv, pass_send, pass_recv, slice_sem, bring_send, bring_recv, keep_sem, table_send,
                  table_recv, chain_send, chain_recv, ready_sem,
                  tail_at, tail_weight, tail_raw, tail_own, tail_up, tail_down, tail_below, tail_above, tail_give_send,
                  tail_give_recv, tail_slice_sem, tail_send, tail_recv, *buffers):
    band, lev = lax.axis_index("lat"), lax.axis_index("lev")
    group, position = band // GROUP, lax.rem(band, GROUP)
    groups = bands // GROUP
    has_up = group < groups - 1
    has_down = group > 0
    rows, field_count, levels, lon_count = fields_ref.shape
    tiles = lon_count // LANES
    tail = tail_of(lon_count)
    last_field = field_count - 1
    count = len(chunks)
    source, mixed = buffers[:count], buffers[count:2 * count]
    column = buffers[2 * count:]
    first_row, total_rows = band * rows, bands * rows
    step_one = 1 - 2 * lax.rem(position, 2)
    step_two = 2 - 4 * (position // 2)
    steps = [step_one, step_two, step_one + step_two]
    partner = {"lev": 1 - lev}
    mates = [{"lat": band + step} for step in steps]
    up_peer, down_peer = {"lat": band + GROUP}, {"lat": band - GROUP}

    loads = [
        pltpu.make_async_copy(fields_ref.at[:, f], held.at[:, f], load_sem.at[f]) for f in range(field_count)
    ]
    loads[0].start()

    def signal(peer):
        pl.semaphore_signal(barrier, inc=1, device_id=peer, device_id_type=MESH)

    barrier = pltpu.get_barrier_semaphore()
    for peer in [partner] + mates[:2]:
        signal(peer)
    pl.when(has_up)(lambda: signal(up_peer))
    pl.when(has_down)(lambda: signal(down_peer))

    scalars = [
        pltpu.make_async_copy(there, here, scalar_sem.at[n])
        for n, (there, here) in enumerate((
            (departure_hbm, departure_ref), (extents_hbm, extents_ref), (lat_t_hbm, lat_t_ref),
            (lon_t_hbm, lon_t_ref), (shift_hbm, shift_ref), (area_hbm, area_ref),
        ))
    ]
    for copy in scalars + loads[1:]:
        copy.start()

    pl.semaphore_wait(barrier, 3 + has_up.astype(jnp.int32) + has_down.astype(jnp.int32))

    def remote(source_ref, target_ref, send_sem, recv_sem, peer):
        return pltpu.make_async_remote_copy(
            src_ref=source_ref, dst_ref=target_ref, send_sem=send_sem, recv_sem=recv_sem,
            device_id=peer, device_id_type=MESH,
        )

    def width_of(f):
        return (lon_count - (tail * LANES if f == last_field else 0)) // GROUP

    def slice_at(home, k):
        f, first, size = chunks[k]
        width = width_of(f)
        return pl.ds(pl.multiple_of(home * width + first, LANES), size)

    def fields_cut(home, k):
        held_first = held if chunks[k][0] == 0 else fields_ref
        return held_first.at[:, chunks[k][0], :, slice_at(home, k)]

    def source_cut(k, n, blocks=1):
        return source[k].at[pl.ds(n * rows, blocks * rows)]

    def column_cut(home, k):
        f, first, size = chunks[k]
        return column[f].at[:, pl.ds((home * width_of(f) + first) // LANES, size // LANES)]

    def note(n, j):
        here, there = ((departure_ref, far_departure), (extents_ref.at[0], far_extents), (lat_t_ref, far_lat))[n]
        slot, peer = ([(position, mate) for mate in mates] + [(GROUP, up_peer), (GROUP + 1, down_peer)])[j]
        return remote(here, there.at[slot], note_send.at[n, j], note_recv.at[n, j], peer)

    def notes(j, act):
        for n in range(3):
            when_z(j - 3, getattr(note(n, j), act))

    def when_z(j, body):
        if j < 0:
            body()
        else:
            pl.when((has_up, has_down)[j])(body)

    def tail_cut():
        return fields_ref.at[:, last_field, :, pl.ds((tiles - tail) * LANES, tail * LANES)]

    def tail_block(member, first=0, size=None):
        size = tail if size is None else size
        return tail_raw.at[pl.ds(member * rows, rows), :, pl.ds(first * LANES, size * LANES)]

    def tail_give(j):
        if j < 2:
            here, there = tail_cut(), tail_block(position)
        else:
            first = (0, tail // 2, tail)[j - 2:j]
            here = there = tail_block(position + steps[j - 2], first[0], first[1] - first[0])
        return remote(here, there, tail_give_send.at[j], tail_give_recv.at[j], mates[(0, 1, 1, 0)[j]])

    tail_slice = pltpu.make_async_copy(tail_cut(), tail_block(position), tail_slice_sem)
    tail_up_copy = remote(tail_up, tail_below, tail_send.at[0], tail_recv.at[0], up_peer)
    tail_down_copy = remote(tail_down, tail_above, tail_send.at[1], tail_recv.at[1], down_peer)

    def give(j, k):
        home = position + steps[j]
        return remote(
            fields_cut(home, k), source_cut(k, GROUP + position), give_send.at[j], give_recv.at[j, k],
            {"lat": band + steps[j]},
        )

    def own_slice(k):
        return pltpu.make_async_copy(fields_cut(position, k), source_cut(k, GROUP + position), slice_sem.at[k])

    def pass_up(k, block, n, blocks=1):
        return remote(block, source_cut(k, n, blocks), pass_send.at[0], pass_recv.at[0, k], up_peer)

    def pass_down(k, block, n, blocks=1):
        return remote(block, source_cut(k, 2 * GROUP + n, blocks), pass_send.at[1], pass_recv.at[1, k], down_peer)

    def pass_on(k, member, block):
        pl.when(has_up)(pass_up(k, block, member).start)
        pl.when(has_down)(pass_down(k, block, member).start)

    def bring(j, k):
        return remote(
            mixed[k].at[pl.ds((position + steps[j]) * rows, rows)], column_cut(position, k),
            bring_send.at[j], bring_recv.at[j, k], {"lat": band + steps[j]},
        )

    def keep(k):
        return pltpu.make_async_copy(
            mixed[k].at[pl.ds(position * rows, rows)], column_cut(position, k), keep_sem.at[k]
        )

    def table_copy(n):
        if n == 0:
            return remote(mine, met.at[0], table_send.at[0], table_recv.at[0], partner)
        return remote(pair, met.at[n], table_send.at[n], table_recv.at[n], mates[n - 1])

    up_copy = remote(upward, below, chain_send.at[0], chain_recv.at[0], up_peer)
    down_copy = remote(downward, above, chain_send.at[1], chain_recv.at[1], down_peer)

    def give_all(k):
        if k < count:
            for j in range(3):
                give(j, k).start()

    def pass_own(k):
        if k < count:
            pass_on(k, position, fields_cut(position, k))

    def take(k):
        if k >= count:
            if k == count:
                tail_combine()
            return
        for j in range(3):
            give(j, k).wait_recv()
            member = position + steps[j]
            pass_on(k, member, source_cut(k, GROUP + member))

    def tail_prepare(n, slot, member_row):
        north, south = far_extents[slot, 0], far_extents[slot, 1]

        def prepare(row, carry):
            departure = departure_of(far_departure[slot, row], north, south, member_row, rows, total_rows)
            for a, weight in enumerate(cubic(far_lat[slot, row])):
                place = departure - 1 + a - group * GROUP * rows
                inside = jnp.logical_and(place >= 0, place < GROUP * rows)
                tail_at[4 * (n * rows + row) + a] = jnp.where(inside, place, 0)
                tail_weight[4 * (n * rows + row) + a] = jnp.where(inside, weight, 0.0)
            return carry

        lax.fori_loop(0, rows, prepare, 0)

    def tail_mix(n, target):
        def one_row(row, carry):
            places = [tail_at[4 * (n * rows + row) + a] for a in range(4)]
            weights = [tail_weight[4 * (n * rows + row) + a] for a in range(4)]
            for t in range(tail):
                at = pl.ds(t * LANES, LANES)
                total = weights[0] * tail_raw[places[0], :, at]
                for a in range(1, 4):
                    total = total + weights[a] * tail_raw[places[a], :, at]
                target[row, t] = total
            return carry

        lax.fori_loop(0, rows, one_row, 0, unroll=2)

    def tail_combine():
        for j in range(2, 4):
            tail_give(j).wait_recv()
        tail_slice.wait()

        @pl.when(has_up)
        def _():
            tail_mix(2, tail_up)
            tail_up_copy.start()

        @pl.when(has_down)
        def _():
            tail_mix(1, tail_down)
            tail_down_copy.start()

        tail_mix(0, tail_own)

        @pl.when(jnp.logical_not(has_down))
        def _():
            tail_below[...] = jnp.zeros_like(tail_below)

        @pl.when(jnp.logical_not(has_up))
        def _():
            tail_above[...] = jnp.zeros_like(tail_above)

    def tail_add():
        pl.when(has_down)(tail_up_copy.wait_recv)
        pl.when(has_up)(tail_down_copy.wait_recv)

        def one_row(row, carry):
            for t in range(tail):
                total = tail_own[row, t] + tail_below[row, t] + tail_above[row, t]
                column[last_field][row, tiles - tail + t] = total
                column[last_field][row, 2 * tiles - tail + t] = total
            return carry

        lax.fori_loop(0, rows, one_row, 0, unroll=2)

    def combine(k):
        own_slice(k).wait()
        pl.when(has_down)(pass_up(k, source_cut(k, 0, GROUP), 0, GROUP).wait_recv)
        pl.when(has_up)(pass_down(k, source_cut(k, 0, GROUP), 0, GROUP).wait_recv)

        def one_row(n, carry):
            first = start_of[n]
            weights = [weight_of[4 * n + a] for a in range(4)]
            for t in range(chunks[k][2] // LANES):
                at = pl.ds(t * LANES, LANES)
                total = weights[0] * source[k][first, :, at]
                for a in range(1, 4):
                    total = total + weights[a] * source[k][first + a, :, at]
                mixed[k][n, t] = total
            return carry

        lax.fori_loop(0, GROUP * rows, one_row, 0, unroll=4)
        for j in range(3):
            bring(j, k).start()
        keep(k).start()

    def chain(hop):
        if hop == 0:
            total = pair[...]
            for n in range(1, 4):
                table_copy(n).wait_recv()
                total = total + met[n]
            plane[...] = total

            @pl.when(jnp.logical_not(has_down))
            def _():
                below[...] = jnp.zeros_like(below)

            @pl.when(jnp.logical_not(has_up))
            def _():
                above[...] = jnp.zeros_like(above)

        @pl.when(group == hop)
        def _():
            if hop > 0:
                up_copy.wait_recv()
            if hop < groups - 1:
                upward[...] = plane[...] + below[...]
                up_copy.start()

        @pl.when(group == groups - 1 - hop)
        def _():
            if hop > 0:
                down_copy.wait_recv()
            if hop < groups - 1:
                downward[...] = plane[...] + above[...]
                down_copy.start()

    def find_ratio():
        total = plane[...] + below[...] + above[...]
        for f in range(field_count):
            sums_at = total[f:f + 1, :]
            mass_before = jnp.sum(sums_at * total[field_count + 1:field_count + 2, :], axis=1, keepdims=True)
            mass_after = jnp.sum(sums_at * total[field_count:field_count + 1, :], axis=1, keepdims=True)
            ratio[f:f + 1, :] = jnp.broadcast_to(mass_before / mass_after, (1, LANES))

    def repeat(f, places):
        def one_row(row, carry):
            for t in places:
                column[f][row, tiles + t] = column[f][row, t]
                if t == 0:
                    column[f][row, 2 * tiles] = column[f][row, t]
            return carry

        lax.fori_loop(0, rows, one_row, 0, unroll=2)

    def along_lon(f):
        for k in range(count):
            if f == last_field and k == count - 1:
                tail_add()
            if chunks[k][0] == f:
                for j in range(3):
                    block = column_cut(position + steps[j], k)
                    remote(block, block, bring_send.at[j], bring_recv.at[j, k], {"lat": band}).wait_recv()
                keep(k).wait()
                first, size = chunks[k][1:]
                starts = [(home * width_of(f) + first) // LANES for home in range(GROUP)]
                repeat(f, [start + t for start in starts for t in range(size // LANES)])
        lane = lax.broadcasted_iota(jnp.int32, (levels, LANES), 1)
        scale = jnp.broadcast_to(ratio[f:f + 1, :], (levels, LANES))

        def one_row(row, carry):
            lon = [lon_of[4 * row + n] * scale for n in range(4)]
            first = lax.rem(shift_ref[row] - 1 + lon_count, lon_count)
            rests = [lax.rem(first + n, LANES) for n in range(4)]
            turns = [lax.rem(LANES - rest, LANES) for rest in rests]
            stays = [lane < LANES - rest for rest in rests]
            bases = [(first + n) // LANES for n in range(4)]

            def turned(t):
                return [pltpu.roll(column[f][row, bases[n] + t], turns[n], 1) for n in range(4)]

            here = turned(0)
            for t in range(tiles):
                there = turned(t + 1)
                total = lon[0] * jnp.where(stays[0], here[0], there[0])
                for n in range(1, 4):
                    total = total + lon[n] * jnp.where(stays[n], here[n], there[n])
                moved_ref[row, f, :, pl.ds(t * LANES, LANES)] = total
                here = there
            return carry

        lax.fori_loop(0, rows, one_row, 0, unroll=ROLL)

    pl.semaphore_signal(ready_sem, inc=1, device_id=mates[0], device_id_type=MESH)
    loads[0].wait()
    pass_own(0)
    for j in range(2):
        give(j, 0).start()
    for k in range(1, OWN):
        pass_own(k)
    pl.semaphore_wait(ready_sem, 1)
    give(2, 0).start()
    for copy in scalars:
        copy.wait()
    for j in range(5):
        notes(j, "start")
    give_all(1)
    for copy in loads[1:]:
        copy.wait()
    lane = lax.broadcasted_iota(jnp.int32, (1, mine.shape[1]), 1)
    taken = jnp.zeros(lane.shape, jnp.float32)
    for row in range(rows):
        departure = departure_of(
            departure_ref[row], extents_ref[0, 0], extents_ref[0, 1], first_row, rows, total_rows
        )
        lon_w = cubic(lon_t_ref[row])
        for n, weight in enumerate(lon_w):
            lon_of[4 * row + n] = weight
        share = area_ref[first_row + row] * (lon_w[0] + lon_w[1] + lon_w[2] + lon_w[3]) * (1.0 / levs)
        for a, weight in enumerate(cubic(lat_t_ref[row])):
            taken = taken + jnp.where(lane == departure - 1 + a, share * weight, 0.0)
    sums = [jnp.zeros(lane.shape, jnp.float32) for _ in range(field_count)]
    before = jnp.zeros(lane.shape, jnp.float32)
    for row in range(rows):
        before = before + jnp.where(lane == first_row + row, area_ref[first_row + row] * (1.0 / levs), 0.0)
        for f in range(field_count):
            total = jnp.sum(jnp.sum(held[row, f], axis=0, keepdims=True), axis=1, keepdims=True)
            sums[f] = sums[f] + jnp.where(lane == first_row + row, total, 0.0)
    mine[...] = jnp.zeros_like(mine)
    for f in range(field_count):
        mine[f:f + 1, :] = sums[f]
    mine[field_count:field_count + 1, :] = taken
    mine[field_count + 1:field_count + 2, :] = before
    table_copy(0).start()
    for k in range(count):
        own_slice(k).start()
    tail_slice.start()
    table_copy(0).wait_recv()
    pair[...] = mine[...] + met[0]
    for n in range(1, 4):
        table_copy(n).start()
    for k in range(2, GIVEN):
        give_all(k)
    for k in range(PASSED):
        take(k)
    for row in range(rows):
        far_departure[position, row] = departure_ref[row]
        far_lat[position, row] = lat_t_ref[row]
    for e in range(2):
        far_extents[position, e] = extents_ref[0, e]
    for n in range(3):
        for j in range(3):
            note(n, j).wait_recv()
        pl.when(has_down)(note(n, 3).wait_recv)
        pl.when(has_up)(note(n, 4).wait_recv)
    for member in range(GROUP):
        member_row = (group * GROUP + member) * rows
        north, south = far_extents[member, 0], far_extents[member, 1]

        def prepare(row, carry):
            departure = departure_of(far_departure[member, row], north, south, member_row, rows, total_rows)
            start_of[member * rows + row] = departure - 1 - (group - 1) * GROUP * rows
            for a, weight in enumerate(cubic(far_lat[member, row])):
                weight_of[4 * (member * rows + row) + a] = weight
            return carry

        lax.fori_loop(0, rows, prepare, 0)
    chain(0)
    tail_prepare(0, position, first_row)
    pl.when(has_down)(lambda: tail_prepare(1, GROUP, first_row - GROUP * rows))
    pl.when(has_up)(lambda: tail_prepare(2, GROUP + 1, first_row + GROUP * rows))

    hop = 1
    finished = 0
    for k in range(count):
        give_all(k + GIVEN)
        pass_own(k + OWN)
        take(k + PASSED)
        if k == TAIL_GIVE:
            for j in range(2):
                tail_give(j).start()
        if k == TAIL_RELAY:
            for j in range(2):
                tail_give(j).wait_recv()
                tail_give(j + 2).start()
        combine(k)
        while hop < groups and (k == count - 1 if hop == groups - 1 else (hop * (count - WAIT)) // groups <= k):
            chain(hop)
            hop += 1
            if hop == groups:
                find_ratio()
        if k < count - 1 and hop == groups and chunks[k - WAIT][0] > finished:
            along_lon(finished)
            finished += 1
    for k in range(count):
        for j in range(3):
            give(j, k).wait_send()
        pl.when(has_up)(pass_up(k, source_cut(k, 0, GROUP), 0, GROUP).wait_send)
        pl.when(has_down)(pass_down(k, source_cut(k, 0, GROUP), 0, GROUP).wait_send)
    for j in range(5):
        notes(j, "wait_send")
    for n in range(4):
        table_copy(n).wait_send()
    for j in range(4):
        tail_give(j).wait_send()
    pl.when(has_up)(up_copy.wait_send)
    pl.when(has_down)(down_copy.wait_send)
    for f in range(finished, field_count):
        along_lon(f)
    for k in range(count):
        for j in range(3):
            bring(j, k).wait_send()
    pl.when(has_up)(tail_up_copy.wait_send)
    pl.when(has_down)(tail_down_copy.wait_send)


def advect(lat_t, lon_t, shift, departure_row, extents, area, fields):
    bands, levs = lax.axis_size("lat"), lax.axis_size("lev")
    rows, field_count, levels, lon_count = fields.shape
    table = (-(-(field_count + 2) // 8) * 8, -(-bands * rows // LANES) * LANES)
    tail = tail_of(lon_count)
    tail_block = pltpu.VMEM((rows, tail, levels, LANES), jnp.float32)
    chunks = chunks_of(field_count, lon_count)
    count = len(chunks)
    dma = pltpu.SemaphoreType.DMA
    hbm = pl.BlockSpec(memory_space=pltpu.HBM)
    operands = (lat_t, lon_t, shift, departure_row, extents, area, fields)
    return pl.pallas_call(
        functools.partial(advect_kernel, bands, levs, chunks),
        out_shape=jax.ShapeDtypeStruct(fields.shape, fields.dtype),
        in_specs=[hbm] * 7,
        out_specs=pl.BlockSpec(memory_space=pltpu.VMEM),
        scratch_shapes=[
            pltpu.SMEM(lat_t.shape, jnp.float32),
            pltpu.SMEM(lon_t.shape, jnp.float32),
            pltpu.SMEM(shift.shape, jnp.int32),
            pltpu.SMEM(departure_row.shape, jnp.int32),
            pltpu.SMEM(extents.shape, jnp.int32),
            pltpu.SMEM(area.shape, jnp.float32),
            pltpu.VMEM(fields.shape, jnp.float32),
            pltpu.SMEM((GROUP + 2, rows), jnp.int32),
            pltpu.SMEM((GROUP + 2, 2), jnp.int32),
            pltpu.SMEM((GROUP + 2, rows), jnp.float32),
            pltpu.SMEM((GROUP * rows,), jnp.int32),
            pltpu.SMEM((4 * GROUP * rows,), jnp.float32),
            pltpu.SMEM((4 * rows,), jnp.float32),
            pltpu.VMEM(table, jnp.float32),
            pltpu.VMEM(table, jnp.float32),
            pltpu.VMEM((4,) + table, jnp.float32),
        ]
        + [pltpu.VMEM(table, jnp.float32)] * 5
        + [
            pltpu.VMEM((table[0], LANES), jnp.float32),
            dma((6,)),
            dma((field_count,)),
            dma((3, 5)),
            dma((3, 5)),
            dma((3,)),
            dma((3, count)),
            dma((2,)),
            dma((2, count)),
            dma((count,)),
            dma((3,)),
            dma((3, count)),
            dma((count,)),
            dma((4,)),
            dma((4,)),
            dma((2,)),
            dma((2,)),
            pltpu.SemaphoreType.REGULAR,
            pltpu.SMEM((12 * rows,), jnp.int32),
            pltpu.SMEM((12 * rows,), jnp.float32),
            pltpu.VMEM((GROUP * rows, levels, tail * LANES), jnp.float32),
        ]
        + [tail_block] * 5
        + [
            dma((4,)),
            dma((4,)),
            dma,
            dma((2,)),
            dma((2,)),
        ]
        + [pltpu.VMEM((3 * GROUP * rows, levels, size), jnp.float32) for _, _, size in chunks]
        + [pltpu.VMEM((GROUP * rows, size // LANES, levels, LANES), jnp.float32) for _, _, size in chunks]
        + [pltpu.VMEM((rows, 2 * lon_count // LANES + 1, levels, LANES), jnp.float32)] * field_count,
        compiler_params=pltpu.CompilerParams(
            collective_id=0, has_side_effects=True, vmem_limit_bytes=VMEM_BYTES
        ),
        name="advect",
    )(*[pltpu.with_memory_space_constraint(x, pltpu.HBM) for x in operands])


def per_device(fields, lat_fraction, lon_fraction, lon_shift, departure_row, extents):
    bands = lax.axis_size("lat")
    total_rows = bands * fields.shape[0]
    row_ids = np.arange(-(-total_rows // LANES) * LANES)
    area = np.where(row_ids < total_rows, np.cos(math.pi * (row_ids + 0.5) / total_rows - math.pi / 2.0), 0.0)
    area = jnp.asarray(area, jnp.float32)
    return advect(lat_fraction, lon_fraction, lon_shift, departure_row, extents, area, fields)


def solution(mesh):
    return jax.shard_map(
        per_device,
        mesh=mesh,
        in_specs=(
            P("lat", None, "lev", None),
            P("lat"),
            P("lat"),
            P("lat"),
            P("lat"),
            P("lat", None),
        ),
        out_specs=P("lat", None, "lev", None),
        check_vma=False,
    )
```

```python
import functools
import math

import jax
import jax.numpy as jnp
import numpy as np
from jax import lax
from jax.experimental import pallas as pl
from jax.experimental.pallas import tpu as pltpu
from jax.sharding import PartitionSpec as P

GROUP = 4
LANES = 128
PARTS = (2, 3, 3)
TAIL = 4
GIVEN = 5
PASSED = 3
WAIT = 1
ROLL = 5
OWN = 3
TAIL_GIVE = 1
TAIL_RELAY = 3
VMEM_BYTES = 40 * 1024 * 1024
MESH = pl.DeviceIdType.MESH


def cubic(t):
    sixth = 1.0 / 6.0
    return (
        -t * (t - 1.0) * (t - 2.0) * sixth,
        (t + 1.0) * (t - 1.0) * (t - 2.0) * 0.5,
        -(t + 1.0) * t * (t - 2.0) * 0.5,
        (t + 1.0) * t * (t - 1.0) * sixth,
    )


def departure_of(departure, north, south, first_row, rows, total_rows):
    low = first_row - north * rows + 1
    high = first_row + rows - 3 + south * rows
    inside = jnp.minimum(jnp.maximum(departure, low), high)
    return jnp.minimum(jnp.maximum(inside, 1), total_rows - 3)


def tail_of(lon_count):
    tiles = lon_count // LANES
    return TAIL + (tiles - TAIL) % GROUP


def chunks_of(field_count, lon_count):
    chunks = []
    for f in range(field_count):
        last = f == field_count - 1
        tiles = (lon_count // LANES - (tail_of(lon_count) if last else 0)) // GROUP
        parts = min(PARTS[min(f, len(PARTS) - 1)], tiles)
        edges = [tiles * n // parts for n in range(parts + 1)]
        if last:
            edges = [tiles - edge for edge in reversed(edges)]
        chunks += [(f, low * LANES, (high - low) * LANES) for low, high in zip(edges, edges[1:])]
    return chunks


def advect_kernel(bands, levs, chunks, lat_t_hbm, lon_t_hbm, shift_hbm, departure_hbm, extents_hbm, area_hbm,
                  fields_ref, moved_ref, lat_t_ref, lon_t_ref, shift_ref, departure_ref, extents_ref,
                  area_ref, held, far_departure, far_extents, far_lat, start_of, weight_of, lon_of, mine, pair, met, plane,
                  below, above, upward, downward, ratio, scalar_sem, load_sem, note_send, note_recv, give_send,
                  give_recv, pass_send, pass_recv, slice_sem, bring_send, bring_recv, keep_sem, table_send,
                  table_recv, chain_send, chain_recv, ready_sem,
                  tail_at, tail_weight, tail_raw, tail_own, tail_up, tail_down, tail_below, tail_above, tail_give_send,
                  tail_give_recv, tail_slice_sem, tail_send, tail_recv, *buffers):
    band, lev = lax.axis_index("lat"), lax.axis_index("lev")
    group, position = band // GROUP, lax.rem(band, GROUP)
    groups = bands // GROUP
    has_up = group < groups - 1
    has_down = group > 0
    rows, field_count, levels, lon_count = fields_ref.shape
    tiles = lon_count // LANES
    tail = tail_of(lon_count)
    last_field = field_count - 1
    count = len(chunks)
    source, mixed = buffers[:count], buffers[count:2 * count]
    column = buffers[2 * count:]
    first_row, total_rows = band * rows, bands * rows
    step_one = 1 - 2 * lax.rem(position, 2)
    step_two = 2 - 4 * (position // 2)
    steps = [step_one, step_two, step_one + step_two]
    partner = {"lev": 1 - lev}
    mates = [{"lat": band + step} for step in steps]
    up_peer, down_peer = {"lat": band + GROUP}, {"lat": band - GROUP}

    loads = [
        pltpu.make_async_copy(fields_ref.at[:, f], held.at[:, f], load_sem.at[f]) for f in range(field_count)
    ]
    loads[0].start()

    def signal(peer):
        pl.semaphore_signal(barrier, inc=1, device_id=peer, device_id_type=MESH)

    barrier = pltpu.get_barrier_semaphore()
    for peer in [partner] + mates[:2]:
        signal(peer)
    pl.when(has_up)(lambda: signal(up_peer))
    pl.when(has_down)(lambda: signal(down_peer))

    scalars = [
        pltpu.make_async_copy(there, here, scalar_sem.at[n])
        for n, (there, here) in enumerate((
            (departure_hbm, departure_ref), (extents_hbm, extents_ref), (lat_t_hbm, lat_t_ref),
            (lon_t_hbm, lon_t_ref), (shift_hbm, shift_ref), (area_hbm, area_ref),
        ))
    ]
    for copy in scalars + loads[1:]:
        copy.start()

    pl.semaphore_wait(barrier, 3 + has_up.astype(jnp.int32) + has_down.astype(jnp.int32))

    def remote(source_ref, target_ref, send_sem, recv_sem, peer):
        return pltpu.make_async_remote_copy(
            src_ref=source_ref, dst_ref=target_ref, send_sem=send_sem, recv_sem=recv_sem,
            device_id=peer, device_id_type=MESH,
        )

    def width_of(f):
        return (lon_count - (tail * LANES if f == last_field else 0)) // GROUP

    def slice_at(home, k):
        f, first, size = chunks[k]
        width = width_of(f)
        return pl.ds(pl.multiple_of(home * width + first, LANES), size)

    def fields_cut(home, k):
        held_first = held if chunks[k][0] == 0 else fields_ref
        return held_first.at[:, chunks[k][0], :, slice_at(home, k)]

    def source_cut(k, n, blocks=1):
        return source[k].at[pl.ds(n * rows, blocks * rows)]

    def column_cut(home, k):
        f, first, size = chunks[k]
        return column[f].at[:, pl.ds((home * width_of(f) + first) // LANES, size // LANES)]

    def note(n, j):
        here, there = ((departure_ref, far_departure), (extents_ref.at[0], far_extents), (lat_t_ref, far_lat))[n]
        slot, peer = ([(position, mate) for mate in mates] + [(GROUP, up_peer), (GROUP + 1, down_peer)])[j]
        return remote(here, there.at[slot], note_send.at[n, j], note_recv.at[n, j], peer)

    def notes(j, act):
        for n in range(3):
            when_z(j - 3, getattr(note(n, j), act))

    def when_z(j, body):
        if j < 0:
            body()
        else:
            pl.when((has_up, has_down)[j])(body)

    def tail_cut():
        return fields_ref.at[:, last_field, :, pl.ds((tiles - tail) * LANES, tail * LANES)]

    def tail_block(member, first=0, size=None):
        size = tail if size is None else size
        return tail_raw.at[pl.ds(member * rows, rows), :, pl.ds(first * LANES, size * LANES)]

    def tail_give(j):
        if j < 2:
            here, there = tail_cut(), tail_block(position)
        else:
            first = (0, tail // 2, tail)[j - 2:j]
            here = there = tail_block(position + steps[j - 2], first[0], first[1] - first[0])
        return remote(here, there, tail_give_send.at[j], tail_give_recv.at[j], mates[(0, 1, 1, 0)[j]])

    tail_slice = pltpu.make_async_copy(tail_cut(), tail_block(position), tail_slice_sem)
    tail_up_copy = remote(tail_up, tail_below, tail_send.at[0], tail_recv.at[0], up_peer)
    tail_down_copy = remote(tail_down, tail_above, tail_send.at[1], tail_recv.at[1], down_peer)

    def give(j, k):
        home = position + steps[j]
        return remote(
            fields_cut(home, k), source_cut(k, GROUP + position), give_send.at[j], give_recv.at[j, k],
            {"lat": band + steps[j]},
        )

    def own_slice(k):
        return pltpu.make_async_copy(fields_cut(position, k), source_cut(k, GROUP + position), slice_sem.at[k])

    def pass_up(k, block, n, blocks=1):
        return remote(block, source_cut(k, n, blocks), pass_send.at[0], pass_recv.at[0, k], up_peer)

    def pass_down(k, block, n, blocks=1):
        return remote(block, source_cut(k, 2 * GROUP + n, blocks), pass_send.at[1], pass_recv.at[1, k], down_peer)

    def pass_on(k, member, block):
        pl.when(has_up)(pass_up(k, block, member).start)
        pl.when(has_down)(pass_down(k, block, member).start)

    def bring(j, k):
        return remote(
            mixed[k].at[pl.ds((position + steps[j]) * rows, rows)], column_cut(position, k),
            bring_send.at[j], bring_recv.at[j, k], {"lat": band + steps[j]},
        )

    def keep(k):
        return pltpu.make_async_copy(
            mixed[k].at[pl.ds(position * rows, rows)], column_cut(position, k), keep_sem.at[k]
        )

    def table_copy(n):
        if n == 0:
            return remote(mine, met.at[0], table_send.at[0], table_recv.at[0], partner)
        return remote(pair, met.at[n], table_send.at[n], table_recv.at[n], mates[n - 1])

    up_copy = remote(upward, below, chain_send.at[0], chain_recv.at[0], up_peer)
    down_copy = remote(downward, above, chain_send.at[1], chain_recv.at[1], down_peer)

    def give_all(k):
        if k < count:
            for j in range(3):
                give(j, k).start()

    def pass_own(k):
        if k < count:
            pass_on(k, position, fields_cut(position, k))

    def take(k):
        if k >= count:
            if k == count:
                tail_combine()
            return
        for j in range(3):
            give(j, k).wait_recv()
            member = position + steps[j]
            pass_on(k, member, source_cut(k, GROUP + member))

    def tail_prepare(n, slot, member_row):
        north, south = far_extents[slot, 0], far_extents[slot, 1]

        def prepare(row, carry):
            departure = departure_of(far_departure[slot, row], north, south, member_row, rows, total_rows)
            for a, weight in enumerate(cubic(far_lat[slot, row])):
                place = departure - 1 + a - group * GROUP * rows
                inside = jnp.logical_and(place >= 0, place < GROUP * rows)
                tail_at[4 * (n * rows + row) + a] = jnp.where(inside, place, 0)
                tail_weight[4 * (n * rows + row) + a] = jnp.where(inside, weight, 0.0)
            return carry

        lax.fori_loop(0, rows, prepare, 0)

    def tail_mix(n, target):
        def one_row(row, carry):
            places = [tail_at[4 * (n * rows + row) + a] for a in range(4)]
            weights = [tail_weight[4 * (n * rows + row) + a] for a in range(4)]
            for t in range(tail):
                at = pl.ds(t * LANES, LANES)
                total = weights[0] * tail_raw[places[0], :, at]
                for a in range(1, 4):
                    total = total + weights[a] * tail_raw[places[a], :, at]
                target[row, t] = total
            return carry

        lax.fori_loop(0, rows, one_row, 0, unroll=5)

    def tail_combine():
        for j in range(2, 4):
            tail_give(j).wait_recv()
        tail_slice.wait()

        @pl.when(has_up)
        def _():
            tail_mix(2, tail_up)
            tail_up_copy.start()

        @pl.when(has_down)
        def _():
            tail_mix(1, tail_down)
            tail_down_copy.start()

        tail_mix(0, tail_own)

        @pl.when(jnp.logical_not(has_down))
        def _():
            tail_below[...] = jnp.zeros_like(tail_below)

        @pl.when(jnp.logical_not(has_up))
        def _():
            tail_above[...] = jnp.zeros_like(tail_above)

    def tail_add():
        pl.when(has_down)(tail_up_copy.wait_recv)
        pl.when(has_up)(tail_down_copy.wait_recv)

        def one_row(row, carry):
            for t in range(tail):
                total = tail_own[row, t] + tail_below[row, t] + tail_above[row, t]
                column[last_field][row, tiles - tail + t] = total
                column[last_field][row, 2 * tiles - tail + t] = total
            return carry

        lax.fori_loop(0, rows, one_row, 0, unroll=5)

    def combine(k):
        own_slice(k).wait()
        pl.when(has_down)(pass_up(k, source_cut(k, 0, GROUP), 0, GROUP).wait_recv)
        pl.when(has_up)(pass_down(k, source_cut(k, 0, GROUP), 0, GROUP).wait_recv)

        def one_row(n, carry):
            first = start_of[n]
            weights = [weight_of[4 * n + a] for a in range(4)]
            for t in range(chunks[k][2] // LANES):
                at = pl.ds(t * LANES, LANES)
                total = weights[0] * source[k][first, :, at]
                for a in range(1, 4):
                    total = total + weights[a] * source[k][first + a, :, at]
                mixed[k][n, t] = total
            return carry

        lax.fori_loop(0, GROUP * rows, one_row, 0, unroll=4)
        for j in range(3):
            bring(j, k).start()
        keep(k).start()

    def chain(hop):
        if hop == 0:
            total = pair[...]
            for n in range(1, 4):
                table_copy(n).wait_recv()
                total = total + met[n]
            plane[...] = total

            @pl.when(jnp.logical_not(has_down))
            def _():
                below[...] = jnp.zeros_like(below)

            @pl.when(jnp.logical_not(has_up))
            def _():
                above[...] = jnp.zeros_like(above)

        @pl.when(group == hop)
        def _():
            if hop > 0:
                up_copy.wait_recv()
            if hop < groups - 1:
                upward[...] = plane[...] + below[...]
                up_copy.start()

        @pl.when(group == groups - 1 - hop)
        def _():
            if hop > 0:
                down_copy.wait_recv()
            if hop < groups - 1:
                downward[...] = plane[...] + above[...]
                down_copy.start()

    def find_ratio():
        total = plane[...] + below[...] + above[...]
        for f in range(field_count):
            sums_at = total[f:f + 1, :]
            mass_before = jnp.sum(sums_at * total[field_count + 1:field_count + 2, :], axis=1, keepdims=True)
            mass_after = jnp.sum(sums_at * total[field_count:field_count + 1, :], axis=1, keepdims=True)
            ratio[f:f + 1, :] = jnp.broadcast_to(mass_before / mass_after, (1, LANES))

    def repeat(f, places):
        def one_row(row, carry):
            for t in places:
                column[f][row, tiles + t] = column[f][row, t]
                if t == 0:
                    column[f][row, 2 * tiles] = column[f][row, t]
            return carry

        lax.fori_loop(0, rows, one_row, 0, unroll=5)

    def along_lon(f):
        for k in range(count):
            if f == last_field and k == count - 1:
                tail_add()
            if chunks[k][0] == f:
                for j in range(3):
                    block = column_cut(position + steps[j], k)
                    remote(block, block, bring_send.at[j], bring_recv.at[j, k], {"lat": band}).wait_recv()
                keep(k).wait()
                first, size = chunks[k][1:]
                starts = [(home * width_of(f) + first) // LANES for home in range(GROUP)]
                repeat(f, [start + t for start in starts for t in range(size // LANES)])
        lane = lax.broadcasted_iota(jnp.int32, (levels, LANES), 1)
        scale = jnp.broadcast_to(ratio[f:f + 1, :], (levels, LANES))

        def one_row(row, carry):
            lon = [lon_of[4 * row + n] * scale for n in range(4)]
            first = lax.rem(shift_ref[row] - 1 + lon_count, lon_count)
            rests = [lax.rem(first + n, LANES) for n in range(4)]
            turns = [lax.rem(LANES - rest, LANES) for rest in rests]
            stays = [lane < LANES - rest for rest in rests]
            bases = [(first + n) // LANES for n in range(4)]

            def turned(t):
                return [pltpu.roll(column[f][row, bases[n] + t], turns[n], 1) for n in range(4)]

            here = turned(0)
            for t in range(tiles):
                there = turned(t + 1)
                total = lon[0] * jnp.where(stays[0], here[0], there[0])
                for n in range(1, 4):
                    total = total + lon[n] * jnp.where(stays[n], here[n], there[n])
                moved_ref[row, f, :, pl.ds(t * LANES, LANES)] = total
                here = there
            return carry

        lax.fori_loop(0, rows, one_row, 0, unroll=ROLL)

    pl.semaphore_signal(ready_sem, inc=1, device_id=mates[0], device_id_type=MESH)
    loads[0].wait()
    pass_own(0)
    for j in range(2):
        give(j, 0).start()
    for k in range(1, OWN):
        pass_own(k)
    pl.semaphore_wait(ready_sem, 1)
    give(2, 0).start()
    for copy in scalars:
        copy.wait()
    for j in range(5):
        notes(j, "start")
    give_all(1)
    for copy in loads[1:]:
        copy.wait()
    lane = lax.broadcasted_iota(jnp.int32, (1, mine.shape[1]), 1)
    taken = jnp.zeros(lane.shape, jnp.float32)
    for row in range(rows):
        departure = departure_of(
            departure_ref[row], extents_ref[0, 0], extents_ref[0, 1], first_row, rows, total_rows
        )
        lon_w = cubic(lon_t_ref[row])
        for n, weight in enumerate(lon_w):
            lon_of[4 * row + n] = weight
        share = area_ref[first_row + row] * (lon_w[0] + lon_w[1] + lon_w[2] + lon_w[3]) * (1.0 / levs)
        for a, weight in enumerate(cubic(lat_t_ref[row])):
            taken = taken + jnp.where(lane == departure - 1 + a, share * weight, 0.0)
    sums = [jnp.zeros(lane.shape, jnp.float32) for _ in range(field_count)]
    before = jnp.zeros(lane.shape, jnp.float32)
    for row in range(rows):
        before = before + jnp.where(lane == first_row + row, area_ref[first_row + row] * (1.0 / levs), 0.0)
        for f in range(field_count):
            total = jnp.sum(jnp.sum(held[row, f], axis=0, keepdims=True), axis=1, keepdims=True)
            sums[f] = sums[f] + jnp.where(lane == first_row + row, total, 0.0)
    mine[...] = jnp.zeros_like(mine)
    for f in range(field_count):
        mine[f:f + 1, :] = sums[f]
    mine[field_count:field_count + 1, :] = taken
    mine[field_count + 1:field_count + 2, :] = before
    table_copy(0).start()
    for k in range(count):
        own_slice(k).start()
    tail_slice.start()
    table_copy(0).wait_recv()
    pair[...] = mine[...] + met[0]
    for n in range(1, 4):
        table_copy(n).start()
    for k in range(2, GIVEN):
        give_all(k)
    for k in range(PASSED):
        take(k)
    for row in range(rows):
        far_departure[position, row] = departure_ref[row]
        far_lat[position, row] = lat_t_ref[row]
    for e in range(2):
        far_extents[position, e] = extents_ref[0, e]
    for n in range(3):
        for j in range(3):
            note(n, j).wait_recv()
        pl.when(has_down)(note(n, 3).wait_recv)
        pl.when(has_up)(note(n, 4).wait_recv)
    for member in range(GROUP):
        member_row = (group * GROUP + member) * rows
        north, south = far_extents[member, 0], far_extents[member, 1]

        def prepare(row, carry):
            departure = departure_of(far_departure[member, row], north, south, member_row, rows, total_rows)
            start_of[member * rows + row] = departure - 1 - (group - 1) * GROUP * rows
            for a, weight in enumerate(cubic(far_lat[member, row])):
                weight_of[4 * (member * rows + row) + a] = weight
            return carry

        lax.fori_loop(0, rows, prepare, 0)
    chain(0)
    tail_prepare(0, position, first_row)
    pl.when(has_down)(lambda: tail_prepare(1, GROUP, first_row - GROUP * rows))
    pl.when(has_up)(lambda: tail_prepare(2, GROUP + 1, first_row + GROUP * rows))

    hop = 1
    finished = 0
    for k in range(count):
        give_all(k + GIVEN)
        pass_own(k + OWN)
        take(k + PASSED)
        if k == TAIL_GIVE:
            for j in range(2):
                tail_give(j).start()
        if k == TAIL_RELAY:
            for j in range(2):
                tail_give(j).wait_recv()
                tail_give(j + 2).start()
        combine(k)
        while hop < groups and (k == count - 1 if hop == groups - 1 else (hop * (count - WAIT)) // groups <= k):
            chain(hop)
            hop += 1
            if hop == groups:
                find_ratio()
        if k < count - 1 and hop == groups and chunks[k - WAIT][0] > finished:
            along_lon(finished)
            finished += 1
    for k in range(count):
        for j in range(3):
            give(j, k).wait_send()
        pl.when(has_up)(pass_up(k, source_cut(k, 0, GROUP), 0, GROUP).wait_send)
        pl.when(has_down)(pass_down(k, source_cut(k, 0, GROUP), 0, GROUP).wait_send)
    for j in range(5):
        notes(j, "wait_send")
    for n in range(4):
        table_copy(n).wait_send()
    for j in range(4):
        tail_give(j).wait_send()
    pl.when(has_up)(up_copy.wait_send)
    pl.when(has_down)(down_copy.wait_send)
    for f in range(finished, field_count):
        along_lon(f)
    for k in range(count):
        for j in range(3):
            bring(j, k).wait_send()
    pl.when(has_up)(tail_up_copy.wait_send)
    pl.when(has_down)(tail_down_copy.wait_send)


def advect(lat_t, lon_t, shift, departure_row, extents, area, fields):
    bands, levs = lax.axis_size("lat"), lax.axis_size("lev")
    rows, field_count, levels, lon_count = fields.shape
    table = (-(-(field_count + 2) // 8) * 8, -(-bands * rows // LANES) * LANES)
    tail = tail_of(lon_count)
    tail_block = pltpu.VMEM((rows, tail, levels, LANES), jnp.float32)
    chunks = chunks_of(field_count, lon_count)
    count = len(chunks)
    dma = pltpu.SemaphoreType.DMA
    hbm = pl.BlockSpec(memory_space=pltpu.HBM)
    operands = (lat_t, lon_t, shift, departure_row, extents, area, fields)
    return pl.pallas_call(
        functools.partial(advect_kernel, bands, levs, chunks),
        out_shape=jax.ShapeDtypeStruct(fields.shape, fields.dtype),
        in_specs=[hbm] * 7,
        out_specs=pl.BlockSpec(memory_space=pltpu.VMEM),
        scratch_shapes=[
            pltpu.SMEM(lat_t.shape, jnp.float32),
            pltpu.SMEM(lon_t.shape, jnp.float32),
            pltpu.SMEM(shift.shape, jnp.int32),
            pltpu.SMEM(departure_row.shape, jnp.int32),
            pltpu.SMEM(extents.shape, jnp.int32),
            pltpu.SMEM(area.shape, jnp.float32),
            pltpu.VMEM(fields.shape, jnp.float32),
            pltpu.SMEM((GROUP + 2, rows), jnp.int32),
            pltpu.SMEM((GROUP + 2, 2), jnp.int32),
            pltpu.SMEM((GROUP + 2, rows), jnp.float32),
            pltpu.SMEM((GROUP * rows,), jnp.int32),
            pltpu.SMEM((4 * GROUP * rows,), jnp.float32),
            pltpu.SMEM((4 * rows,), jnp.float32),
            pltpu.VMEM(table, jnp.float32),
            pltpu.VMEM(table, jnp.float32),
            pltpu.VMEM((4,) + table, jnp.float32),
        ]
        + [pltpu.VMEM(table, jnp.float32)] * 5
        + [
            pltpu.VMEM((table[0], LANES), jnp.float32),
            dma((6,)),
            dma((field_count,)),
            dma((3, 5)),
            dma((3, 5)),
            dma((3,)),
            dma((3, count)),
            dma((2,)),
            dma((2, count)),
            dma((count,)),
            dma((3,)),
            dma((3, count)),
            dma((count,)),
            dma((4,)),
            dma((4,)),
            dma((2,)),
            dma((2,)),
            pltpu.SemaphoreType.REGULAR,
            pltpu.SMEM((12 * rows,), jnp.int32),
            pltpu.SMEM((12 * rows,), jnp.float32),
            pltpu.VMEM((GROUP * rows, levels, tail * LANES), jnp.float32),
        ]
        + [tail_block] * 5
        + [
            dma((4,)),
            dma((4,)),
            dma,
            dma((2,)),
            dma((2,)),
        ]
        + [pltpu.VMEM((3 * GROUP * rows, levels, size), jnp.float32) for _, _, size in chunks]
        + [pltpu.VMEM((GROUP * rows, size // LANES, levels, LANES), jnp.float32) for _, _, size in chunks]
        + [pltpu.VMEM((rows, 2 * lon_count // LANES + 1, levels, LANES), jnp.float32)] * field_count,
        compiler_params=pltpu.CompilerParams(
            collective_id=0, has_side_effects=True, vmem_limit_bytes=VMEM_BYTES
        ),
        name="advect",
    )(*[pltpu.with_memory_space_constraint(x, pltpu.HBM) for x in operands])


def per_device(fields, lat_fraction, lon_fraction, lon_shift, departure_row, extents):
    bands = lax.axis_size("lat")
    total_rows = bands * fields.shape[0]
    row_ids = np.arange(-(-total_rows // LANES) * LANES)
    area = np.where(row_ids < total_rows, np.cos(math.pi * (row_ids + 0.5) / total_rows - math.pi / 2.0), 0.0)
    area = jnp.asarray(area, jnp.float32)
    return advect(lat_fraction, lon_fraction, lon_shift, departure_row, extents, area, fields)


def solution(mesh):
    return jax.shard_map(
        per_device,
        mesh=mesh,
        in_specs=(
            P("lat", None, "lev", None),
            P("lat"),
            P("lat"),
            P("lat"),
            P("lat"),
            P("lat", None),
        ),
        out_specs=P("lat", None, "lev", None),
        check_vma=False,
    )
```
